8 devices in a mesh: dp: 2 (over z, y), tp: 4 (over x, core).
Axes of the slice: x: 2, y: 2, z: 1, core: 2. Of those that a mesh axis runs over, the one named last changes fastest.
Arguments:
- x: bfloat16 [2, 2048, 1536], P('dp', 'tp')
- dy: bfloat16 [2, 2048, 1536], P('dp', 'tp')
- wq: bfloat16 [1536, 2048], P('dp', 'tp')
- wk: bfloat16 [1536, 2048], P('dp', 'tp')
- wv: bfloat16 [1536, 2048], P('dp', 'tp')
- wo: bfloat16 [2048, 1536], P(('tp', 'dp'))
- w_gate: bfloat16 [1536, 12288], P('dp', 'tp')
- w_up: bfloat16 [1536, 12288], P('dp', 'tp')
- w_down: bfloat16 [12288, 1536], P(('tp', 'dp'))
Outputs:
- output 1: bfloat16 [2, 2048, 1536], P('dp', 'tp')
- output 2: bfloat16 [1536, 2048], P('dp', 'tp')
- output 3: bfloat16 [1536, 2048], P('dp', 'tp')
- output 4: bfloat16 [1536, 2048], P('dp', 'tp')
- output 5: bfloat16 [2048, 1536], P(('tp', 'dp'))
- output 6: bfloat16 [1536, 12288], P('dp', 'tp')
- output 7: bfloat16 [1536, 12288], P('dp', 'tp')
- output 8: bfloat16 [12288, 1536], P(('tp', 'dp'))
All inputs are finite; a program needn't handle non-finite values.
Results may differ from the reference program's by a relative error of at most 0.024.
Values are sent between devices in bfloat16 or wider.
A program may use at most 2 GiB of HBM per device.

```python
import jax
import jax.numpy as jnp
from jax import lax

SEQUENCES = 2
TOKENS = 2048
D = 1536
HEADS = 8
KV_HEADS = 8
HEAD = 256
FF = 12288
THETA = 10000
NAMES = ("wq", "wk", "wv", "wo", "w_gate", "w_up", "w_down")
SHAPES = {
    "wq": (D, HEADS * HEAD),
    "wk": (D, KV_HEADS * HEAD),
    "wv": (D, KV_HEADS * HEAD),
    "wo": (HEADS * HEAD, D),
    "w_gate": (D, FF),
    "w_up": (D, FF),
    "w_down": (FF, D),
}


def bump(key, n, height):
    away = (jnp.arange(n, dtype=jnp.int32) - jax.random.randint(key, (), 0, n, jnp.int32)) % n
    return jnp.where(away < n // 8, height, 1.0)


def together(key, own, strength):
    shared = jax.random.normal(key, own.shape[1:], jnp.float32)
    return (own + strength * shared) * lax.rsqrt(1 + strength * strength)


def setup_inputs(seed: int = 0, part: int = 0) -> dict:
    kx, kdy, ka, kb, kz, kf, kh, kl, *kw = jax.random.split(jax.random.key(seed), 8 + len(NAMES))
    shape = (SEQUENCES, TOKENS, D)
    much_x, much_dy = jax.random.uniform(kz, (2,), jnp.float32, 0.0, 1.0)
    loud = 2.0 ** jax.random.uniform(jax.random.fold_in(kz, 1), (), jnp.float32, -1.0, 2.0)
    halves = 2.0 ** jax.random.uniform(kl, (2,), jnp.float32, -1.0, 1.0)
    times = {"wq": 1.0, "wk": 1.0, "wv": 2.0, "wo": halves[0], "w_gate": 1.0, "w_up": bump(kh, FF, 4.0), "w_down": halves[1]}
    x = together(ka, jax.random.normal(kx, shape, jnp.float32), much_x) * bump(kf, D, 4.0)
    dy = together(kb, jax.random.normal(kdy, shape, jnp.float32), much_dy)
    drawn = {"x": x.astype(jnp.bfloat16), "dy": (loud * dy * (SEQUENCES * TOKENS) ** -0.5).astype(jnp.bfloat16)}
    for key, name in zip(kw, NAMES, strict=True):
        drawn[name] = (jax.random.normal(key, SHAPES[name], jnp.float32) * SHAPES[name][0] ** -0.5 * times[name]).astype(jnp.bfloat16)
    return drawn


def matmul(a, w):
    return jnp.dot(a, w, preferred_element_type=jnp.float32).astype(jnp.bfloat16)


def normed(h):
    wide = h.astype(jnp.float32)
    scale = lax.rsqrt(jnp.mean(wide**2, -1, keepdims=True) + 1e-6)
    return (wide * scale).astype(jnp.bfloat16)


def turned(t, theta):
    half = t.shape[-1] // 2
    angle = jnp.arange(t.shape[0], dtype=jnp.float32)[:, None] * theta ** (-jnp.arange(half, dtype=jnp.float32) / half)
    cos, sin = jnp.cos(angle)[:, None], jnp.sin(angle)[:, None]
    a, b = t[..., :half].astype(jnp.float32), t[..., half:].astype(jnp.float32)
    return jnp.concatenate([a * cos - b * sin, b * cos + a * sin], -1).astype(jnp.bfloat16)


def seen_by(q, k, v):
    tokens, kv = q.shape[0], k.shape[1]
    q = q.reshape(tokens, kv, -1, q.shape[-1])
    scores = jnp.einsum("tgsd,ugd->gstu", q.astype(jnp.float32), k.astype(jnp.float32)) * q.shape[-1] ** -0.5
    place = jnp.arange(tokens)
    weights = jax.nn.softmax(jnp.where(place[:, None] >= place, scores, -jnp.inf), -1).astype(jnp.bfloat16)
    return jnp.einsum("gstu,ugd->tgsd", weights.astype(jnp.float32), v.astype(jnp.float32)).astype(jnp.bfloat16).reshape(tokens, -1)


def layer(h, w):
    a = normed(h)
    q, k = (turned(matmul(a, w[name]).reshape(h.shape[0], -1, HEAD), THETA) for name in ("wq", "wk"))
    h = h + matmul(seen_by(q, k, matmul(a, w["wv"]).reshape(h.shape[0], -1, HEAD)), w["wo"])
    b = normed(h)
    gate = jnp.dot(b, w["w_gate"], preferred_element_type=jnp.float32)
    up = jnp.dot(b, w["w_up"], preferred_element_type=jnp.float32)
    return h + matmul((jax.nn.silu(gate) * up).astype(jnp.bfloat16), w["w_down"])


def reference(x, dy, wq, wk, wv, wo, w_gate, w_up, w_down):
    weights = dict(zip(NAMES, (wq, wk, wv, wo, w_gate, w_up, w_down), strict=True))

    def take(so_far, sequence):
        h, by_y = sequence
        _, back = jax.vjp(lambda w, h: layer(h, w), weights, h)
        by_weights, by_h = back(by_y)
        return jax.tree.map(lambda total, term: total + term.astype(jnp.float32), so_far, by_weights), by_h

    none_yet = {name: jnp.zeros(w.shape, jnp.float32) for name, w in weights.items()}
    by_weights, by_x = lax.scan(take, none_yet, (x, dy))
    return (by_x, *(by_weights[name].astype(jnp.bfloat16) for name in NAMES))
```

```python
import functools

import jax
import jax.numpy as jnp
from jax import lax
from jax.experimental import pallas as pl
from jax.experimental.pallas import tpu as pltpu
from jax.sharding import PartitionSpec as P

HEAD = 256
HALF = HEAD // 2
THETA = 10000
LOG2E = 1.4426950408889634
HIDDEN = -1e30
VMEM = 58 * 2**20


def _dot(a, b, ca, cb):
    return lax.dot_general(a, b, (((ca,), (cb,)), ((), ())), preferred_element_type=jnp.float32)


def _turn(t, cos, sin):
    a, b = t[:, :HALF].astype(jnp.float32), t[:, HALF:].astype(jnp.float32)
    return jnp.concatenate([a * cos - b * sin, b * cos + a * sin], -1).astype(jnp.bfloat16)


def _turn_back(t, cos, sin):
    a, b = t[:, :HALF], t[:, HALF:]
    return jnp.concatenate([a * cos + b * sin, b * cos - a * sin], -1).astype(jnp.bfloat16)


def _mask(n):
    return lax.broadcasted_iota(jnp.int32, (n, n), 1) >= lax.broadcasted_iota(jnp.int32, (n, n), 0)


def _fwd_kernel(q_ref, k_ref, v_ref, cos_ref, sin_ref, o_ref, lse_ref, k_s, *, strip):
    tokens = q_ref.shape[0]
    e = HEAD**-0.5 * LOG2E
    ok = _mask(strip)
    for i in range(tokens // strip):
        here = pl.ds(i * strip, strip)
        cos, sin = cos_ref[here, :], sin_ref[here, :]
        q = _turn(q_ref[here, :], cos, sin)
        k_s[here, :] = _turn(k_ref[here, :], cos, sin)
        n = i * strip
        diag = jnp.where(ok, _dot(k_s[here, :], q, 1, 1), HIDDEN)
        top = diag.max(axis=0, keepdims=True)
        if n:
            past = _dot(k_s[:n, :], q, 1, 1)
            top = jnp.maximum(top, past.max(axis=0, keepdims=True))
        p = jnp.exp2((diag - top) * e)
        total = p.sum(axis=0, keepdims=True)
        out = _dot(v_ref[here, :], p.astype(jnp.bfloat16), 0, 0)
        if n:
            p = jnp.exp2((past - top) * e)
            total += p.sum(axis=0, keepdims=True)
            out += _dot(v_ref[:n, :], p.astype(jnp.bfloat16), 0, 0)
        o_ref[here, :] = (out * (1 / total)).T.astype(jnp.bfloat16)
        lse_ref[0, :, here] = top * e + jnp.log2(total)


def attend(qkv, cos, sin, strip=512):
    tokens, heads = qkv.shape[0], qkv.shape[1] // HEAD // 3
    column = lambda first: pl.BlockSpec((tokens, HEAD), lambda h: (0, first + h))
    whole = pl.BlockSpec((tokens, HALF), lambda h: (0, 0))
    return pl.pallas_call(
        functools.partial(_fwd_kernel, strip=strip),
        grid=(heads,),
        in_specs=[column(0), column(heads), column(2 * heads), whole, whole],
        out_specs=[column(0), pl.BlockSpec((1, 1, tokens), lambda h: (h, 0, 0))],
        out_shape=[jax.ShapeDtypeStruct((tokens, heads * HEAD), jnp.bfloat16), jax.ShapeDtypeStruct((heads, 1, tokens), jnp.float32)],
        scratch_shapes=[pltpu.VMEM((tokens, HEAD), jnp.bfloat16)],
        compiler_params=pltpu.CompilerParams(dimension_semantics=("arbitrary",), vmem_limit_bytes=VMEM),
        cost_estimate=pl.CostEstimate(flops=4 * heads * tokens * tokens * HEAD, transcendentals=heads * tokens * tokens, bytes_accessed=4 * tokens * heads * HEAD * 2),
    )(qkv, qkv, qkv, cos, sin)


def _bwd_kernel(q_ref, k_ref, v_ref, do_ref, lse_ref, cos_ref, sin_ref, dq_ref, dk_ref, dv_ref, k_s, dk_s, dv_s, *, strip):
    tokens = q_ref.shape[0]
    scale = HEAD**-0.5
    e = scale * LOG2E
    ok = _mask(strip)
    for i in range(tokens // strip):
        here = pl.ds(i * strip, strip)
        cos, sin = cos_ref[here, :], sin_ref[here, :]
        q = _turn(q_ref[here, :], cos, sin)
        k_s[here, :] = _turn(k_ref[here, :], cos, sin)
        do, lse = do_ref[here, :], lse_ref[0, :, here]
        n = i * strip
        p = jnp.where(ok, jnp.exp2(_dot(k_s[here, :], q, 1, 1) * e - lse), 0.0)
        dp = _dot(v_ref[here, :], do, 1, 1)
        delta = (p * dp).sum(axis=0, keepdims=True)
        if n:
            p0 = jnp.exp2(_dot(k_s[:n, :], q, 1, 1) * e - lse)
            dp0 = _dot(v_ref[:n, :], do, 1, 1)
            delta += (p0 * dp0).sum(axis=0, keepdims=True)
        ds = (p * (dp - delta)).astype(jnp.bfloat16)
        dv_s[here, :] = _dot(p.astype(jnp.bfloat16), do, 1, 0)
        dk_s[here, :] = _dot(ds, q, 1, 0)
        dq = _dot(ds, k_s[here, :], 0, 0)
        if n:
            ds0 = (p0 * (dp0 - delta)).astype(jnp.bfloat16)
            dv_s[:n, :] += _dot(p0.astype(jnp.bfloat16), do, 1, 0)
            dk_s[:n, :] += _dot(ds0, q, 1, 0)
            dq += _dot(ds0, k_s[:n, :], 0, 0)
        dq_ref[here, :] = _turn_back(dq * scale, cos, sin)
    for i in range(tokens // strip):
        here = pl.ds(i * strip, strip)
        dk_ref[here, :] = _turn_back(dk_s[here, :] * scale, cos_ref[here, :], sin_ref[here, :])
        dv_ref[here, :] = dv_s[here, :].astype(jnp.bfloat16)


def attend_bwd(qkv, d_out, lse, cos, sin, strip=512):
    tokens, heads = qkv.shape[0], qkv.shape[1] // HEAD // 3
    column = lambda first: pl.BlockSpec((tokens, HEAD), lambda h: (0, first + h))
    whole = pl.BlockSpec((tokens, HALF), lambda h: (0, 0))
    return pl.pallas_call(
        functools.partial(_bwd_kernel, strip=strip),
        grid=(heads,),
        in_specs=[column(0), column(heads), column(2 * heads), column(0), pl.BlockSpec((1, 1, tokens), lambda h: (h, 0, 0)), whole, whole],
        out_specs=[column(0)] * 3,
        out_shape=[jax.ShapeDtypeStruct((tokens, heads * HEAD), jnp.bfloat16)] * 3,
        scratch_shapes=[pltpu.VMEM((tokens, HEAD), jnp.bfloat16), pltpu.VMEM((tokens, HEAD), jnp.float32), pltpu.VMEM((tokens, HEAD), jnp.float32)],
        compiler_params=pltpu.CompilerParams(dimension_semantics=("arbitrary",), vmem_limit_bytes=VMEM),
        cost_estimate=pl.CostEstimate(flops=10 * heads * tokens * tokens * HEAD, transcendentals=heads * tokens * tokens, bytes_accessed=7 * tokens * heads * HEAD * 2),
    )(qkv, qkv, qkv, d_out, lse, cos, sin)


def _ffn_kernel(b_ref, dh_ref, w_ref, hid_ref, dgu_ref, db_ref, *, piece):
    units = dh_ref.shape[1]
    b = b_ref[...]
    for at in range(0, units, piece):
        g = _dot(b, w_ref[:, at : at + piece], 1, 0)
        u = _dot(b, w_ref[:, units + at : units + at + piece], 1, 0)
        dh = dh_ref[:, at : at + piece].astype(jnp.float32)
        s = jax.nn.sigmoid(g)
        gs = g * s
        hid_ref[:, at : at + piece] = (gs * u).astype(jnp.bfloat16)
        dgu_ref[:, at : at + piece] = (dh * u * (s + gs * (1 - s))).astype(jnp.bfloat16)
        dgu_ref[:, units + at : units + at + piece] = (dh * gs).astype(jnp.bfloat16)
    db_ref[...] = _dot(dgu_ref[...], w_ref[...], 1, 1).astype(jnp.bfloat16)


def ffn(b, d_hidden, w, rows=256, piece=512):
    tokens, d = b.shape
    units = d_hidden.shape[1]
    row = lambda n: pl.BlockSpec((rows, n), lambda i: (i, 0))
    return pl.pallas_call(
        functools.partial(_ffn_kernel, piece=piece),
        grid=(tokens // rows,),
        in_specs=[row(d), row(units), pl.BlockSpec((d, 2 * units), lambda i: (0, 0), pipeline_mode=pl.Buffered(1))],
        out_specs=[row(units), row(2 * units), row(d)],
        out_shape=[jax.ShapeDtypeStruct((tokens, n), jnp.bfloat16) for n in (units, 2 * units, d)],
        compiler_params=pltpu.CompilerParams(dimension_semantics=("arbitrary",), vmem_limit_bytes=VMEM),
        cost_estimate=pl.CostEstimate(flops=8 * tokens * d * units, transcendentals=tokens * units, bytes_accessed=2 * (tokens * (2 * d + 4 * units) + 2 * d * units)),
    )(b, d_hidden, w)


def bf16(t):
    return t.astype(jnp.bfloat16)


def f32(t):
    return t.astype(jnp.float32)


def normed(h):
    wide = f32(h)
    scale = lax.rsqrt(jnp.mean(wide**2, -1, keepdims=True) + 1e-6)
    return bf16(wide * scale)


def normed_bwd(h, by):
    wide, by = f32(h), f32(by)
    scale = lax.rsqrt(jnp.mean(wide**2, -1, keepdims=True) + 1e-6)
    return scale * (by - wide * (scale * scale * jnp.mean(by * wide, -1, keepdims=True)))


def solution(mesh):
    def step(x, dy, wq, wk, wv, wo, wg, wu, wd):
        d = lax.axis_index("dp")
        x, dy = x[0], dy[0]
        tokens = x.shape[0] * mesh.shape["tp"]
        width, units = x.shape[1], wd.shape[0]
        swap = lambda t: lax.ppermute(t, "dp", [(0, 1), (1, 0)])
        gather = lambda t: lax.all_gather(t, "tp", axis=0, tiled=True)
        scatter = lambda t: lax.psum_scatter(t, "tp", scatter_dimension=0, tiled=True)
        flip = lambda t: jnp.where(d == 0, t, jnp.concatenate([t[:, width // 2 :], t[:, : width // 2]], 1))
        mine = lambda w: lax.dynamic_slice_in_dim(w, d * units, units, axis=1)
        theirs = lambda w: lax.dynamic_slice_in_dim(w, (1 - d) * units, units, axis=1)

        qkv_mine = jnp.concatenate([wq, wk, wv], 1)
        w_qkv = jnp.concatenate([qkv_mine, swap(qkv_mine)], 0)
        wo_theirs = swap(wo)
        w_o = jnp.where(d == 0, jnp.concatenate([wo, wo_theirs], 0), jnp.concatenate([wo_theirs, wo], 0))
        gu_theirs = swap(jnp.concatenate([theirs(wg), theirs(wu)], 1))
        w_gu = jnp.concatenate([jnp.concatenate([mine(wg), mine(wu)], 1), gu_theirs], 0)

        angle = jnp.arange(tokens, dtype=jnp.float32)[:, None] * THETA ** (-jnp.arange(HALF, dtype=jnp.float32) / HALF)
        cos, sin = jnp.cos(angle), jnp.sin(angle)

        a = gather(flip(normed(x)))
        qkv = bf16(_dot(a, w_qkv, 1, 0))
        heads, lse = attend(qkv, cos, sin)
        h = bf16(f32(x) + f32(scatter(bf16(_dot(heads, w_o, 1, 0)))))

        dys = [gather(dy), gather(swap(dy))]
        d_hidden = [bf16(_dot(t, wd, 1, 1)) for t in dys]
        b = normed(h)
        bs = [gather(flip(b)), gather(flip(swap(b)))]
        done = [ffn(t, dh, w_gu) for t, dh in zip(bs, d_hidden)]
        (hid0, dgu0, db0), (hid1, dgu1, db1) = done
        back1 = swap(flip(scatter(db1)))
        db = f32(flip(scatter(db0))) + f32(back1)
        gu_half = lambda lo: bf16(_dot(bs[0][:, lo : lo + width // 2], dgu0, 0, 0) + _dot(bs[1][:, lo : lo + width // 2], dgu1, 0, 0))
        send_gu = swap(gu_half(width // 2))
        keep_gu = gu_half(0)
        d_wd = bf16(_dot(hid0, dys[0], 0, 0) + _dot(hid1, dys[1], 0, 0))
        join = lambda own, other: jnp.where(d == 0, jnp.concatenate([own, other], 1), jnp.concatenate([other, own], 1))
        d_wg = join(keep_gu[:, :units], send_gu[:, :units])
        d_wu = join(keep_gu[:, units:], send_gu[:, units:])

        dh = bf16(f32(dy) + f32(bf16(normed_bwd(h, bf16(db)))))
        dh_all = gather(dh)
        d_heads = bf16(_dot(dh_all, w_o, 1, 1))
        d_wo_all = _dot(heads, dh_all, 0, 0)
        rows = wo.shape[0]
        wo_part = lambda i: lax.dynamic_slice_in_dim(d_wo_all, i * rows, rows, axis=0)
        d_wo = bf16(wo_part(d) + f32(swap(bf16(wo_part(1 - d)))))
        d_qkv = jnp.concatenate(attend_bwd(qkv, d_heads, lse, cos, sin), 1)
        d_w = lambda lo: _dot(a[:, lo : lo + width // 2], d_qkv, 0, 0)
        d_w_qkv = bf16(d_w(0) + f32(swap(bf16(d_w(width // 2)))))
        da = flip(scatter(bf16(_dot(d_qkv, w_qkv, 1, 1))))
        dx = bf16(f32(dh) + f32(bf16(normed_bwd(x, da))))
        cols = wq.shape[1]
        return dx[None], d_w_qkv[:, :cols], d_w_qkv[:, cols : 2 * cols], d_w_qkv[:, 2 * cols :], d_wo, d_wg, d_wu, d_wd

    states, by_columns, by_rows = P("dp", "tp", None), P("dp", "tp"), P(("tp", "dp"), None)
    weights = (by_columns, by_columns, by_columns, by_rows, by_columns, by_columns, by_rows)
    return jax.shard_map(step, mesh=mesh, in_specs=(states, states, *weights), out_specs=(states, *weights), check_vma=False)
```

```python
import functools

import jax
import jax.numpy as jnp
from jax import lax
from jax.experimental import pallas as pl
from jax.experimental.pallas import tpu as pltpu
from jax.sharding import PartitionSpec as P

HEAD = 256
HALF = HEAD // 2
THETA = 10000
LOG2E = 1.4426950408889634
HIDDEN = -1e30
VMEM = 58 * 2**20


def _dot(a, b, ca, cb):
    return lax.dot_general(a, b, (((ca,), (cb,)), ((), ())), preferred_element_type=jnp.float32)


def _turn(t, cos, sin):
    a, b = t[:, :HALF].astype(jnp.float32), t[:, HALF:].astype(jnp.float32)
    return jnp.concatenate([a * cos - b * sin, b * cos + a * sin], -1).astype(jnp.bfloat16)


def _turn_back(t, cos, sin):
    a, b = t[:, :HALF], t[:, HALF:]
    return jnp.concatenate([a * cos + b * sin, b * cos - a * sin], -1).astype(jnp.bfloat16)


def _mask(n):
    return lax.broadcasted_iota(jnp.int32, (n, n), 1) >= lax.broadcasted_iota(jnp.int32, (n, n), 0)


def _fwd_kernel(qkv_ref, cos_ref, sin_ref, o_ref, lse_ref, k_s, *, strip):
    tokens = qkv_ref.shape[0]
    q_ref, k_ref, v_ref = (qkv_ref.at[:, i * HEAD : (i + 1) * HEAD] for i in range(3))
    e = HEAD**-0.5 * LOG2E
    ok = _mask(strip)
    for i in range(tokens // strip):
        here = pl.ds(i * strip, strip)
        cos, sin = cos_ref[here, :], sin_ref[here, :]
        q = _turn(q_ref[here, :], cos, sin)
        k_s[here, :] = _turn(k_ref[here, :], cos, sin)
        n = i * strip
        diag = jnp.where(ok, _dot(k_s[here, :], q, 1, 1), HIDDEN)
        top = diag.max(axis=0, keepdims=True)
        if n:
            past = _dot(k_s[:n, :], q, 1, 1)
            top = jnp.maximum(top, past.max(axis=0, keepdims=True))
        p = jnp.exp2((diag - top) * e)
        total = p.sum(axis=0, keepdims=True)
        out = _dot(v_ref[here, :], p.astype(jnp.bfloat16), 0, 0)
        if n:
            p = jnp.exp2((past - top) * e)
            total += p.sum(axis=0, keepdims=True)
            out += _dot(v_ref[:n, :], p.astype(jnp.bfloat16), 0, 0)
        o_ref[here, :] = (out * (1 / total)).T.astype(jnp.bfloat16)
        lse_ref[0, :, here] = top * e + jnp.log2(total)


def attend(qkv, cos, sin, strip=512):
    tokens, heads = qkv.shape[0], qkv.shape[1] // HEAD // 3
    column = lambda n: pl.BlockSpec((tokens, n * HEAD), lambda h: (0, h))
    whole = pl.BlockSpec((tokens, HALF), lambda h: (0, 0))
    return pl.pallas_call(
        functools.partial(_fwd_kernel, strip=strip),
        grid=(heads,),
        in_specs=[column(3), whole, whole],
        out_specs=[column(1), pl.BlockSpec((1, 1, tokens), lambda h: (h, 0, 0))],
        out_shape=[jax.ShapeDtypeStruct((tokens, heads * HEAD), jnp.bfloat16), jax.ShapeDtypeStruct((heads, 1, tokens), jnp.float32)],
        scratch_shapes=[pltpu.VMEM((tokens, HEAD), jnp.bfloat16)],
        compiler_params=pltpu.CompilerParams(dimension_semantics=("arbitrary",), vmem_limit_bytes=VMEM),
        cost_estimate=pl.CostEstimate(flops=4 * heads * tokens * tokens * HEAD, transcendentals=heads * tokens * tokens, bytes_accessed=4 * tokens * heads * HEAD * 2),
    )(qkv, cos, sin)


def _bwd_kernel(qkv_ref, do_ref, lse_ref, cos_ref, sin_ref, dqkv_ref, k_s, dk_s, dv_s, *, strip):
    tokens = qkv_ref.shape[0]
    q_ref, k_ref, v_ref = (qkv_ref.at[:, i * HEAD : (i + 1) * HEAD] for i in range(3))
    dq_ref, dk_ref, dv_ref = (dqkv_ref.at[:, i * HEAD : (i + 1) * HEAD] for i in range(3))
    scale = HEAD**-0.5
    e = scale * LOG2E
    ok = _mask(strip)
    for i in range(tokens // strip):
        here = pl.ds(i * strip, strip)
        cos, sin = cos_ref[here, :], sin_ref[here, :]
        q = _turn(q_ref[here, :], cos, sin)
        k_s[here, :] = _turn(k_ref[here, :], cos, sin)
        do, lse = do_ref[here, :], lse_ref[0, :, here]
        n = i * strip
        p = jnp.where(ok, jnp.exp2(_dot(k_s[here, :], q, 1, 1) * e - lse), 0.0)
        dp = _dot(v_ref[here, :], do, 1, 1)
        delta = (p * dp).sum(axis=0, keepdims=True)
        if n:
            p0 = jnp.exp2(_dot(k_s[:n, :], q, 1, 1) * e - lse)
            dp0 = _dot(v_ref[:n, :], do, 1, 1)
            delta += (p0 * dp0).sum(axis=0, keepdims=True)
        ds = (p * (dp - delta)).astype(jnp.bfloat16)
        dv_s[here, :] = _dot(p.astype(jnp.bfloat16), do, 1, 0)
        dk_s[here, :] = _dot(ds, q, 1, 0)
        dq = _dot(ds, k_s[here, :], 0, 0)
        if n:
            ds0 = (p0 * (dp0 - delta)).astype(jnp.bfloat16)
            dv_s[:n, :] += _dot(p0.astype(jnp.bfloat16), do, 1, 0)
            dk_s[:n, :] += _dot(ds0, q, 1, 0)
            dq += _dot(ds0, k_s[:n, :], 0, 0)
        dq_ref[here, :] = _turn_back(dq * scale, cos, sin)
    for i in range(tokens // strip):
        here = pl.ds(i * strip, strip)
        dk_ref[here, :] = _turn_back(dk_s[here, :] * scale, cos_ref[here, :], sin_ref[here, :])
        dv_ref[here, :] = dv_s[here, :].astype(jnp.bfloat16)


def attend_bwd(qkv, d_out, lse, cos, sin, strip=512):
    tokens, heads = qkv.shape[0], qkv.shape[1] // HEAD // 3
    column = lambda n: pl.BlockSpec((tokens, n * HEAD), lambda h: (0, h))
    whole = pl.BlockSpec((tokens, HALF), lambda h: (0, 0))
    return pl.pallas_call(
        functools.partial(_bwd_kernel, strip=strip),
        grid=(heads,),
        in_specs=[column(3), column(1), pl.BlockSpec((1, 1, tokens), lambda h: (h, 0, 0)), whole, whole],
        out_specs=column(3),
        out_shape=jax.ShapeDtypeStruct(qkv.shape, jnp.bfloat16),
        scratch_shapes=[pltpu.VMEM((tokens, HEAD), jnp.bfloat16), pltpu.VMEM((tokens, HEAD), jnp.float32), pltpu.VMEM((tokens, HEAD), jnp.float32)],
        compiler_params=pltpu.CompilerParams(dimension_semantics=("arbitrary",), vmem_limit_bytes=VMEM),
        cost_estimate=pl.CostEstimate(flops=10 * heads * tokens * tokens * HEAD, transcendentals=heads * tokens * tokens, bytes_accessed=7 * tokens * heads * HEAD * 2),
    )(qkv, d_out, lse, cos, sin)


BLOCK = 256


def _params(n=1):
    return pltpu.CompilerParams(dimension_semantics=("arbitrary",) * n, vmem_limit_bytes=VMEM)


def _pair(k, n, m):
    return pl.BlockSpec((BLOCK, n), lambda i, *_: (jnp.clip(i - k * m, 0, m - 1), 0))


def _kept(shape):
    return pl.BlockSpec(shape, lambda i, *_: (0, 0), pipeline_mode=pl.Buffered(1))


def _cost(flops, arrays):
    return pl.CostEstimate(flops=flops, transcendentals=0, bytes_accessed=sum(a.size * a.dtype.itemsize for a in arrays))


def _rows_kernel(pos_ref, a_ref, b_ref, *rest, work, m, n_w, n_out):
    w_refs, outs = rest[:n_w], rest[-n_out:]

    @pl.when(pl.program_id(0) < m)
    def _():
        work(a_ref, w_refs, outs, pos_ref)

    @pl.when(pl.program_id(0) >= m)
    def _():
        work(b_ref, w_refs, outs, pos_ref)


def rows_into(work, a, b, weights, places, total, widths, buffers=None, extra=(), flops=0):
    rows = a.shape[0]
    m = rows // BLOCK
    pos = jnp.stack([jnp.asarray(p, jnp.int32) for p in places])
    out = lambda n: pl.BlockSpec((BLOCK, n), lambda i, pos: (pos[i // m] * m + i % m, 0))
    n_fixed = 3 + len(weights)
    given = list(buffers or ())
    return pl.pallas_call(
        functools.partial(_rows_kernel, work=work, m=m, n_w=len(weights), n_out=len(widths)),
        grid_spec=pltpu.PrefetchScalarGridSpec(
            num_scalar_prefetch=1,
            grid=(2 * m,),
            in_specs=[_pair(0, a.shape[1], m), _pair(1, b.shape[1], m), *(_kept(w.shape) for w in weights), *(pl.BlockSpec(memory_space=pl.ANY) for _ in given)],
            out_specs=[out(n) for n in widths],
        ),
        out_shape=[jax.ShapeDtypeStruct((total, n), jnp.bfloat16) for n in widths],
        input_output_aliases={n_fixed + i: i for i in range(len(given))},
        compiler_params=_params(),
        cost_estimate=_cost(flops, [a, b, *weights]),
    )(pos, a, b, *weights, *given)


def bf16(t):
    return t.astype(jnp.bfloat16)


def f32(t):
    return t.astype(jnp.float32)


def _project(a_ref, w_refs, outs, pos_ref):
    first, second = w_refs
    k = first.shape[0]
    outs[0][...] = bf16(_dot(a_ref[:, :k], first[...], 1, 0) + _dot(a_ref[:, k:], second[...], 1, 0))
    outs[1][...] = a_ref[...]


def _hidden_back_kernel(a_ref, b_ref, w_ref, *rest, m):
    out_ref, copy_ref = rest[-2:]

    def work(x_ref):
        out_ref[...] = bf16(_dot(x_ref[...], w_ref[...], 1, 1))
        copy_ref[...] = x_ref[...]

    @pl.when(pl.program_id(0) < m)
    def _():
        work(a_ref)

    @pl.when(pl.program_id(0) >= m)
    def _():
        work(b_ref)


def hidden_back(a, b, w, n, total, buffer):
    rows, d = a.shape
    m = rows // BLOCK
    given = [] if buffer is None else [buffer]
    return pl.pallas_call(
        functools.partial(_hidden_back_kernel, m=m),
        grid=(2 * m,),
        in_specs=[_pair(0, d, m), _pair(1, d, m), _kept(w.shape), *(pl.BlockSpec(memory_space=pl.ANY) for _ in given)],
        out_specs=[pl.BlockSpec((BLOCK, w.shape[0]), lambda i: (i, 0)), pl.BlockSpec((BLOCK, d), lambda i: (n * 2 * m + i, 0))],
        out_shape=[jax.ShapeDtypeStruct((2 * rows, w.shape[0]), jnp.bfloat16), jax.ShapeDtypeStruct((total, d), jnp.bfloat16)],
        input_output_aliases={3: 1} if given else {},
        compiler_params=_params(),
        cost_estimate=_cost(4 * rows * d * w.shape[0], [a, b, w]),
    )(a, b, w, *given)


def _heads_back(a_ref, w_refs, outs, pos_ref):
    a = a_ref[...]
    n = w_refs[0].shape[0]
    for j, w in enumerate(w_refs):
        place = pos_ref[2] if j == 0 else 1 - pos_ref[2]
        outs[0][:, pl.ds(pl.multiple_of(place * n, n), n)] = bf16(_dot(a, w[...], 1, 1))
    outs[1][...] = a


def _from_kernel(pos_ref, *refs, turned, n_in):
    ins, (w1, w2), outs = refs[:n_in], refs[n_in : n_in + 2], refs[n_in + 2 :]

    def put(o_ref):
        if turned:
            n = w1.shape[0]
            a = ins[0][...]
            o_ref[:, :n] = bf16(_dot(a, w1[...], 1, 1))
            o_ref[:, n:] = bf16(_dot(a, w2[...], 1, 1))
        else:
            o_ref[...] = bf16(_dot(ins[0][...], w1[...], 1, 0) + _dot(ins[1][...], w2[...], 1, 0))

    m = pl.num_programs(0) // 2

    @pl.when(pl.program_id(0) < m)
    def _():
        put(outs[0])

    @pl.when(pl.program_id(0) >= m)
    def _():
        put(outs[1])


def rows_from(t, w1, w2, places, rows, width, order=None):
    m = rows // BLOCK
    turned = order is None
    pos = jnp.stack([jnp.asarray(p, jnp.int32) for p in (*places, 0 if turned else order)])
    row = lambda i, pos: pos[i // m] * m + i % m
    if turned:
        ins = [pl.BlockSpec((BLOCK, t.shape[1]), lambda i, pos: (row(i, pos), 0))]
    else:
        half = t.shape[1] // 2
        ins = [pl.BlockSpec((BLOCK, half), lambda i, pos: (row(i, pos), pos[2])), pl.BlockSpec((BLOCK, half), lambda i, pos: (row(i, pos), 1 - pos[2]))]
    return pl.pallas_call(
        functools.partial(_from_kernel, turned=turned, n_in=len(ins)),
        grid_spec=pltpu.PrefetchScalarGridSpec(
            num_scalar_prefetch=1, grid=(2 * m,), in_specs=[*ins, _kept(w1.shape), _kept(w2.shape)], out_specs=[_pair(0, width, m), _pair(1, width, m)]
        ),
        out_shape=[jax.ShapeDtypeStruct((rows, width), jnp.bfloat16)] * 2,
        compiler_params=_params(),
        cost_estimate=_cost(4 * rows * t.shape[1] * width, [w1, w2]),
    )(pos, *([t] * len(ins)), w1, w2)


def _ffn_kernel(a_ref, b_ref, dh_ref, w1_ref, w2_ref, *rest, piece, m):
    hid_ref, dgu_ref, in_ref, da_ref, db_ref = rest[-5:]
    units = dh_ref.shape[1]
    k = w1_ref.shape[0]

    def work(x_ref, dx_ref):
        x1, x2 = x_ref[:, :k], x_ref[:, k:]
        in_ref[...] = x_ref[...]
        for at in range(0, units, piece):
            here, there = slice(at, at + piece), slice(units + at, units + at + piece)
            g = _dot(x1, w1_ref[:, here], 1, 0) + _dot(x2, w2_ref[:, here], 1, 0)
            u = _dot(x1, w1_ref[:, there], 1, 0) + _dot(x2, w2_ref[:, there], 1, 0)
            dh = f32(dh_ref[:, here])
            s = jax.nn.sigmoid(g)
            gs = g * s
            hid_ref[:, here] = bf16(gs * u)
            dgu_ref[:, here] = bf16(dh * u * (s + gs * (1 - s)))
            dgu_ref[:, there] = bf16(dh * gs)
        dx_ref[:, :k] = bf16(_dot(dgu_ref[...], w1_ref[...], 1, 1))
        dx_ref[:, k:] = bf16(_dot(dgu_ref[...], w2_ref[...], 1, 1))

    @pl.when(pl.program_id(0) < m)
    def _():
        work(a_ref, da_ref)

    @pl.when(pl.program_id(0) >= m)
    def _():
        work(b_ref, db_ref)


def ffn(a, b, d_hidden, w1, w2, n, total, buffers, piece=512):
    rows, d = a.shape
    units = d_hidden.shape[1]
    m = rows // BLOCK
    at = lambda width: pl.BlockSpec((BLOCK, width), lambda i: (n * 2 * m + i, 0))
    given = list(buffers or ())
    widths = (units, 2 * units, d)
    *buffers, da, db = pl.pallas_call(
        functools.partial(_ffn_kernel, piece=piece, m=m),
        grid=(2 * m,),
        in_specs=[_pair(0, d, m), _pair(1, d, m), pl.BlockSpec((BLOCK, units), lambda i: (i, 0)), _kept(w1.shape), _kept(w2.shape), *(pl.BlockSpec(memory_space=pl.ANY) for _ in given)],
        out_specs=[*(at(w) for w in widths), _pair(0, d, m), _pair(1, d, m)],
        out_shape=[*(jax.ShapeDtypeStruct((total, w), jnp.bfloat16) for w in widths), *[jax.ShapeDtypeStruct((rows, d), jnp.bfloat16)] * 2],
        input_output_aliases={5 + i: i for i in range(len(given))},
        compiler_params=_params(),
        cost_estimate=_cost(16 * rows * d * units, [a, b, w1, w2]),
    )(a, b, d_hidden, w1, w2, *given)
    return buffers, da, db


def normed(h):
    wide = f32(h)
    scale = lax.rsqrt(jnp.mean(wide**2, -1, keepdims=True) + 1e-6)
    return bf16(wide * scale)


def normed_bwd(h, by):
    wide, by = f32(h), f32(by)
    scale = lax.rsqrt(jnp.mean(wide**2, -1, keepdims=True) + 1e-6)
    return scale * (by - wide * (scale * scale * jnp.mean(by * wide, -1, keepdims=True)))


CORE, OVER_X, OVER_Y = ("tp", ((0, 1), (1, 0), (2, 3), (3, 2))), ("tp", ((0, 2), (1, 3), (2, 0), (3, 1))), ("dp", ((0, 1), (1, 0)))


def send(way, t):
    return lax.ppermute(t, way[0], way[1])


def layer(x, dy, wq, wk, wv, wo, wg, wu, wd):
    d, t = lax.axis_index("dp"), lax.axis_index("tp")
    own, width = x.shape
    seq, units = 4 * own, wd.shape[0]
    half = width // 2
    t_core, t_x = t + 1 - 2 * lax.rem(t, 2), lax.rem(t + 2, 4)
    t_xcore = t_x + 1 - 2 * lax.rem(t, 2)
    flip = lambda t: jnp.where(d == 0, t, jnp.concatenate([t[:, half:], t[:, :half]], 1))
    other = lambda t: jnp.concatenate([t[:, half:], t[:, :half]], 1)
    mine = lambda w: lax.dynamic_slice_in_dim(w, d * units, units, axis=1)
    theirs = lambda w: lax.dynamic_slice_in_dim(w, (1 - d) * units, units, axis=1)
    heads_n = wq.shape[1] // HEAD

    a = flip(normed(x))
    qkv_mine = jnp.concatenate([w[:, i * HEAD : (i + 1) * HEAD] for i in range(heads_n) for w in (wq, wk, wv)], 1)
    qkv_theirs = send(OVER_Y, qkv_mine)
    ax = send(OVER_X, a)
    ac = send(CORE, a)
    gu_send = jnp.concatenate([theirs(wg), theirs(wu)], 1)
    gu_mine = jnp.concatenate([mine(wg), mine(wu)], 1)
    wo_theirs = send(OVER_Y, wo)
    gu_theirs = send(OVER_Y, gu_send)
    axc = send(CORE, ax)

    dyc = send(CORE, dy)
    dyx = send(OVER_X, dy)
    dyxc = send(CORE, dyx)
    dyy = send(OVER_Y, dy)
    dyyc = send(CORE, dyy)
    dyd = send(OVER_X, dyy)
    dydc = send(CORE, dyd)

    angle = jnp.arange(seq, dtype=jnp.float32)[:, None] * THETA ** (-jnp.arange(HALF, dtype=jnp.float32) / HALF)
    cos, sin = jnp.cos(angle), jnp.sin(angle)

    proj = functools.partial(rows_into, _project, weights=(qkv_mine, qkv_theirs), total=seq, widths=(qkv_mine.shape[1], width), flops=4 * own * width * qkv_mine.shape[1])
    kept = proj(a, ac, places=(t, t_core))
    qkv, a_all = proj(ax, axc, places=(t_x, t_xcore), buffers=kept)
    heads, lse = attend(qkv, cos, sin)
    o_from = functools.partial(rows_from, heads, wo, wo_theirs, rows=own, width=width, order=d)
    ox, oxc = o_from(places=(t_x, t_xcore))
    sox = bf16(f32(ox) + f32(send(CORE, oxc)))
    o_far = send(OVER_X, sox)
    o, oc = o_from(places=(t, t_core))
    o_near = send(CORE, oc)
    h = bf16(f32(x) + f32(bf16(f32(o) + f32(o_near) + f32(o_far))))
    b = normed(h)
    b_mine = flip(b)

    by = send(OVER_Y, other(b_mine))
    bx = send(OVER_X, b_mine)
    bc = send(CORE, b_mine)
    bxc = send(CORE, bx)
    byc = send(CORE, by)
    bd = send(OVER_X, by)
    bdc = send(CORE, bd)
    dy_all, d_hid = None, []
    for n, (u, v) in enumerate(((dy, dyc), (dyx, dyxc), (dyy, dyyc), (dyd, dydc))):
        part, dy_all = hidden_back(u, v, wd, n, 2 * seq, dy_all)
        d_hid.append(part)
    kept, sums = None, []
    for n, (u, v) in enumerate(((b_mine, bc), (bx, bxc), (by, byc), (bd, bdc))):
        kept, du, dv = ffn(u, v, d_hid[n], gu_mine, gu_theirs, n, 2 * seq, kept)
        near = send(CORE, dv)
        sums.append(f32(du) + f32(near))
    hid, dgu, b_all = kept
    s_own, s_x, s_y, s_d = sums
    cut = own // 2
    s_d = bf16(s_d)
    e_lo, e_hi = send(OVER_X, s_d[:cut]), send(OVER_Y, other(s_d[cut:]))
    fx_lo, fy_hi = send(OVER_X, bf16(s_x[:cut])), send(OVER_Y, other(bf16(s_y[cut:])))
    fx_hi = send(OVER_X, bf16(s_x[cut:] + f32(e_hi)))
    fy_lo = send(OVER_Y, other(bf16(s_y[:cut] + f32(e_lo))))
    far = jnp.concatenate([f32(fx_lo) + f32(fy_lo), f32(fx_hi) + f32(fy_hi)], 0)
    db = bf16(flip(s_own + far))
    dh = bf16(f32(dy) + f32(bf16(normed_bwd(h, db))))

    gu_part = bf16(_dot(b_all[:, half:], dgu, 0, 0))
    gu_got = send(OVER_Y, gu_part)
    gu_kept = bf16(_dot(b_all[:, :half], dgu, 0, 0))
    d_wd = bf16(_dot(hid, dy_all, 0, 0))

    dhx = send(OVER_X, dh)
    dhc = send(CORE, dh)
    dhxc = send(CORE, dhx)
    heads_back = functools.partial(rows_into, _heads_back, weights=(wo, wo_theirs), total=seq, widths=(heads.shape[1], width), flops=4 * own * width * heads.shape[1])
    kept = heads_back(dh, dhc, places=(t, t_core, d))
    d_heads, dh_all = heads_back(dhx, dhxc, places=(t_x, t_xcore, d), buffers=kept)
    d_qkv = attend_bwd(qkv, d_heads, lse, cos, sin)
    qkv_part = bf16(_dot(a_all[:, half:], d_qkv, 0, 0))
    qkv_got = send(OVER_Y, qkv_part)
    a_from = functools.partial(rows_from, d_qkv, qkv_mine, qkv_theirs, rows=own, width=width)
    dax, daxc = a_from(places=(t_x, t_xcore))
    sdax = bf16(f32(dax) + f32(send(CORE, daxc)))
    da_far = send(OVER_X, sdax)
    da, dac = a_from(places=(t, t_core))
    da_near = send(CORE, dac)
    d_wo_all = bf16(_dot(heads, dh_all, 0, 0))
    rows = wo.shape[0]
    wo_part = lambda i: lax.dynamic_slice_in_dim(d_wo_all, i * rows, rows, axis=0)
    wo_send = wo_part(1 - d)
    wo_got = send(OVER_Y, wo_send)
    qkv_kept = lax.optimization_barrier(_dot(a_all[:, :half], d_qkv, 0, 0))
    join = lambda u, v: jnp.where(d == 0, jnp.concatenate([u, v], 1), jnp.concatenate([v, u], 1))
    d_wg = join(gu_kept[:, :units], gu_got[:, :units])
    d_wu = join(gu_kept[:, units:], gu_got[:, units:])
    d_wo = bf16(f32(wo_part(d)) + f32(wo_got))
    da_sum = bf16(flip(f32(da) + f32(da_near) + f32(da_far)))
    dx = bf16(f32(dh) + f32(bf16(normed_bwd(x, da_sum))))
    cols = lambda j: [slice((3 * i + j) * HEAD, (3 * i + j + 1) * HEAD) for i in range(heads_n)]
    col = lambda j: jnp.concatenate([bf16(qkv_kept[:, at] + f32(qkv_got[:, at])) for at in cols(j)], 1)
    return dx, col(0), col(1), col(2), d_wo, d_wg, d_wu, d_wd


def solution(mesh):
    def step(x, dy, *weights):
        dx, *rest = layer(x[0], dy[0], *weights)
        return (dx[None], *rest)

    states, by_columns, by_rows = P("dp", "tp", None), P("dp", "tp"), P(("tp", "dp"), None)
    weights = (by_columns, by_columns, by_columns, by_rows, by_columns, by_columns, by_rows)
    return jax.shard_map(step, mesh=mesh, in_specs=(states, states, *weights), out_specs=(states, *weights), check_vma=False)
```

```python
import functools

import jax
import jax.numpy as jnp
from jax import lax
from jax.experimental import pallas as pl
from jax.experimental.pallas import tpu as pltpu
from jax.sharding import PartitionSpec as P

HEAD = 256
HALF = HEAD // 2
THETA = 10000
LOG2E = 1.4426950408889634
HIDDEN = -1e30
VMEM = 58 * 2**20


def _dot(a, b, ca, cb):
    return lax.dot_general(a, b, (((ca,), (cb,)), ((), ())), preferred_element_type=jnp.float32)


def _turn(t, cos, sin):
    a, b = t[:, :HALF].astype(jnp.float32), t[:, HALF:].astype(jnp.float32)
    return jnp.concatenate([a * cos - b * sin, b * cos + a * sin], -1).astype(jnp.bfloat16)


def _turn_back(t, cos, sin):
    a, b = t[:, :HALF], t[:, HALF:]
    return jnp.concatenate([a * cos + b * sin, b * cos - a * sin], -1).astype(jnp.bfloat16)


def _mask(n):
    return lax.broadcasted_iota(jnp.int32, (n, n), 1) >= lax.broadcasted_iota(jnp.int32, (n, n), 0)


def _fwd_kernel(q_ref, k_ref, v_ref, cos_ref, sin_ref, o_ref, lse_ref, k_s, *, strip):
    tokens = q_ref.shape[0]
    e = HEAD**-0.5 * LOG2E
    ok = _mask(strip)
    for i in range(tokens // strip):
        here = pl.ds(i * strip, strip)
        cos, sin = cos_ref[here, :], sin_ref[here, :]
        q = _turn(q_ref[here, :], cos, sin)
        k_s[here, :] = _turn(k_ref[here, :], cos, sin)
        n = i * strip
        diag = jnp.where(ok, _dot(k_s[here, :], q, 1, 1), HIDDEN)
        top = diag.max(axis=0, keepdims=True)
        if n:
            past = _dot(k_s[:n, :], q, 1, 1)
            top = jnp.maximum(top, past.max(axis=0, keepdims=True))
        p = jnp.exp2((diag - top) * e)
        total = p.sum(axis=0, keepdims=True)
        out = _dot(v_ref[here, :], p.astype(jnp.bfloat16), 0, 0)
        if n:
            p = jnp.exp2((past - top) * e)
            total += p.sum(axis=0, keepdims=True)
            out += _dot(v_ref[:n, :], p.astype(jnp.bfloat16), 0, 0)
        o_ref[here, :] = (out * (1 / total)).T.astype(jnp.bfloat16)
        lse_ref[0, :, here] = top * e + jnp.log2(total)


def attend(q, k, v, cos, sin, strip=512):
    tokens, heads = q.shape[0], q.shape[1] // HEAD
    column = pl.BlockSpec((tokens, HEAD), lambda h: (0, h))
    whole = pl.BlockSpec((tokens, HALF), lambda h: (0, 0))
    return pl.pallas_call(
        functools.partial(_fwd_kernel, strip=strip),
        grid=(heads,),
        in_specs=[column, column, column, whole, whole],
        out_specs=[column, pl.BlockSpec((1, 1, tokens), lambda h: (h, 0, 0))],
        out_shape=[jax.ShapeDtypeStruct((tokens, heads * HEAD), jnp.bfloat16), jax.ShapeDtypeStruct((heads, 1, tokens), jnp.float32)],
        scratch_shapes=[pltpu.VMEM((tokens, HEAD), jnp.bfloat16)],
        compiler_params=pltpu.CompilerParams(dimension_semantics=("arbitrary",), vmem_limit_bytes=VMEM),
        cost_estimate=pl.CostEstimate(flops=4 * heads * tokens * tokens * HEAD, transcendentals=heads * tokens * tokens, bytes_accessed=4 * tokens * heads * HEAD * 2),
    )(q, k, v, cos, sin)


def _bwd_kernel(q_ref, k_ref, v_ref, do_ref, lse_ref, cos_ref, sin_ref, out_ref, k_s, dk_s, dv_s, *, strip):
    tokens = q_ref.shape[0]
    scale = HEAD**-0.5
    e = scale * LOG2E

    def put(j, rows, t):
        at = (j * pl.num_programs(0) + pl.program_id(0)) * HEAD
        out_ref[rows, pl.ds(pl.multiple_of(at, HEAD), HEAD)] = t

    ok = _mask(strip)
    for i in range(tokens // strip):
        here = pl.ds(i * strip, strip)
        cos, sin = cos_ref[here, :], sin_ref[here, :]
        q = _turn(q_ref[here, :], cos, sin)
        k_s[here, :] = _turn(k_ref[here, :], cos, sin)
        do, lse = do_ref[here, :], lse_ref[0, :, here]
        n = i * strip
        p = jnp.where(ok, jnp.exp2(_dot(k_s[here, :], q, 1, 1) * e - lse), 0.0)
        dp = _dot(v_ref[here, :], do, 1, 1)
        delta = (p * dp).sum(axis=0, keepdims=True)
        if n:
            p0 = jnp.exp2(_dot(k_s[:n, :], q, 1, 1) * e - lse)
            dp0 = _dot(v_ref[:n, :], do, 1, 1)
            delta += (p0 * dp0).sum(axis=0, keepdims=True)
        ds = (p * (dp - delta)).astype(jnp.bfloat16)
        dv_s[here, :] = _dot(p.astype(jnp.bfloat16), do, 1, 0)
        dk_s[here, :] = _dot(ds, q, 1, 0)
        dq = _dot(ds, k_s[here, :], 0, 0)
        if n:
            ds0 = (p0 * (dp0 - delta)).astype(jnp.bfloat16)
            dv_s[:n, :] += _dot(p0.astype(jnp.bfloat16), do, 1, 0)
            dk_s[:n, :] += _dot(ds0, q, 1, 0)
            dq += _dot(ds0, k_s[:n, :], 0, 0)
        put(0, here, _turn_back(dq * scale, cos, sin))
    for i in range(tokens // strip):
        here = pl.ds(i * strip, strip)
        put(1, here, _turn_back(dk_s[here, :] * scale, cos_ref[here, :], sin_ref[here, :]))
        put(2, here, dv_s[here, :].astype(jnp.bfloat16))


def attend_bwd(q, k, v, d_out, lse, cos, sin, strip=512):
    tokens, heads = q.shape[0], q.shape[1] // HEAD
    column = pl.BlockSpec((tokens, HEAD), lambda h: (0, h))
    whole = pl.BlockSpec((tokens, HALF), lambda h: (0, 0))
    return pl.pallas_call(
        functools.partial(_bwd_kernel, strip=strip),
        grid=(heads,),
        in_specs=[column, column, column, column, pl.BlockSpec((1, 1, tokens), lambda h: (h, 0, 0)), whole, whole],
        out_specs=pl.BlockSpec((tokens, 3 * heads * HEAD), lambda h: (0, 0), pipeline_mode=pl.Buffered(1)),
        out_shape=jax.ShapeDtypeStruct((tokens, 3 * heads * HEAD), jnp.bfloat16),
        scratch_shapes=[pltpu.VMEM((tokens, HEAD), jnp.bfloat16), pltpu.VMEM((tokens, HEAD), jnp.float32), pltpu.VMEM((tokens, HEAD), jnp.float32)],
        compiler_params=pltpu.CompilerParams(dimension_semantics=("arbitrary",), vmem_limit_bytes=VMEM),
        cost_estimate=pl.CostEstimate(flops=10 * heads * tokens * tokens * HEAD, transcendentals=heads * tokens * tokens, bytes_accessed=7 * tokens * heads * HEAD * 2),
    )(q, k, v, d_out, lse, cos, sin)


BLOCK = 256


def _params(n=1):
    return pltpu.CompilerParams(dimension_semantics=("arbitrary",) * n, vmem_limit_bytes=VMEM)


def _pair(k, n, m):
    return pl.BlockSpec((BLOCK, n), lambda i, *_: (jnp.clip(i - k * m, 0, m - 1), 0))


def _kept(shape):
    return pl.BlockSpec(shape, lambda i, *_: (0, 0), pipeline_mode=pl.Buffered(1))


def _cost(flops, arrays):
    return pl.CostEstimate(flops=flops, transcendentals=0, bytes_accessed=sum(a.size * a.dtype.itemsize for a in arrays))


def _rows_kernel(pos_ref, *refs, work, m, n_in, n_w, n_out):
    for k in range(n_in):

        @pl.when(pl.program_id(0) // m == k)
        def _(k=k):
            work(refs[k], refs[n_in : n_in + n_w], refs[-n_out:], pos_ref)


def rows_into(work, arrays, weights, places, total, widths, buffers=None, flops=0):
    rows, n_in = arrays[0].shape[0], len(arrays)
    m = rows // BLOCK
    pos = jnp.stack([jnp.asarray(p, jnp.int32) for p in places])
    out = lambda n: pl.BlockSpec((BLOCK, n), lambda i, pos: (pos[i // m] * m + i % m, 0))
    given = list(buffers or ())
    return pl.pallas_call(
        functools.partial(_rows_kernel, work=work, m=m, n_in=n_in, n_w=len(weights), n_out=len(widths)),
        grid_spec=pltpu.PrefetchScalarGridSpec(
            num_scalar_prefetch=1,
            grid=(n_in * m,),
            in_specs=[*(_pair(k, a.shape[1], m) for k, a in enumerate(arrays)), *(_kept(w.shape) for w in weights), *(pl.BlockSpec(memory_space=pl.ANY) for _ in given)],
            out_specs=[out(n) for n in widths],
        ),
        out_shape=[jax.ShapeDtypeStruct((total, n), jnp.bfloat16) for n in widths],
        input_output_aliases={1 + n_in + len(weights) + i: i for i in range(len(given))},
        compiler_params=_params(),
        cost_estimate=_cost(flops, [*arrays, *weights]),
    )(pos, *arrays, *weights, *given)


def bf16(t):
    return t.astype(jnp.bfloat16)


def f32(t):
    return t.astype(jnp.float32)


def _project(a_ref, w_refs, outs, pos_ref):
    k = w_refs[0].shape[0]
    for out, first, second in zip(outs, w_refs[::2], w_refs[1::2]):
        out[...] = bf16(_dot(a_ref[:, :k], first[...], 1, 0) + _dot(a_ref[:, k:], second[...], 1, 0))
    outs[-2][...], outs[-1][...] = a_ref[:, :k], a_ref[:, k:]


def _hidden_back_kernel(a_ref, b_ref, w_ref, *rest, m):
    out_ref, copy_ref = rest[-2:]

    def work(x_ref):
        out_ref[...] = bf16(_dot(x_ref[...], w_ref[...], 1, 1))
        copy_ref[...] = x_ref[...]

    @pl.when(pl.program_id(0) < m)
    def _():
        work(a_ref)

    @pl.when(pl.program_id(0) >= m)
    def _():
        work(b_ref)


def hidden_back(a, b, w, n, total, buffer):
    rows, d = a.shape
    m = rows // BLOCK
    given = [] if buffer is None else [buffer]
    return pl.pallas_call(
        functools.partial(_hidden_back_kernel, m=m),
        grid=(2 * m,),
        in_specs=[_pair(0, d, m), _pair(1, d, m), _kept(w.shape), *(pl.BlockSpec(memory_space=pl.ANY) for _ in given)],
        out_specs=[pl.BlockSpec((BLOCK, w.shape[0]), lambda i: (i, 0)), pl.BlockSpec((BLOCK, d), lambda i: (n * 2 * m + i, 0))],
        out_shape=[jax.ShapeDtypeStruct((2 * rows, w.shape[0]), jnp.bfloat16), jax.ShapeDtypeStruct((total, d), jnp.bfloat16)],
        input_output_aliases={3: 1} if given else {},
        compiler_params=_params(),
        cost_estimate=_cost(4 * rows * d * w.shape[0], [a, b, w]),
    )(a, b, w, *given)


def _heads_back(a_ref, w_refs, outs, pos_ref):
    a = a_ref[...]
    n = w_refs[0].shape[0]
    for j, w in enumerate(w_refs):
        place = pos_ref[4] if j == 0 else 1 - pos_ref[4]
        outs[0][:, pl.ds(pl.multiple_of(place * n, n), n)] = bf16(_dot(a, w[...], 1, 1))
    outs[1][...] = a


def _from_kernel(pos_ref, *refs, turned, n_in, n_w):
    ins, w_refs, outs = refs[:n_in], refs[n_in : n_in + n_w], refs[n_in + n_w :]

    def put(o_ref):
        if turned:
            n = w_refs[0].shape[0]
            for j in range(2):
                o_ref[:, j * n : (j + 1) * n] = bf16(sum(_dot(a[...], w[...], 1, 1) for a, w in zip(ins, w_refs[j::2])))
        else:
            o_ref[...] = bf16(sum(_dot(a[...], w[...], 1, 0) for a, w in zip(ins, w_refs)))

    m = pl.num_programs(0) // len(outs)
    for k, o_ref in enumerate(outs):

        @pl.when(pl.program_id(0) // m == k)
        def _(o_ref=o_ref):
            put(o_ref)


def rows_from(t, weights, places, rows, width, order=None):
    m, n = rows // BLOCK, len(places)
    turned = order is None
    pos = jnp.stack([jnp.asarray(p, jnp.int32) for p in (*places, 0 if turned else order)])
    parts = len(weights) // 2 if turned else 2
    wide = t.shape[1] // parts
    column = lambda j, pos: j if turned else pos[n] if j == 0 else 1 - pos[n]
    ins = [pl.BlockSpec((BLOCK, wide), lambda i, pos, j=j: (pos[i // m] * m + i % m, column(j, pos))) for j in range(parts)]
    return pl.pallas_call(
        functools.partial(_from_kernel, turned=turned, n_in=parts, n_w=len(weights)),
        grid_spec=pltpu.PrefetchScalarGridSpec(
            num_scalar_prefetch=1,
            grid=(n * m,),
            in_specs=[*ins, *(_kept(w.shape) for w in weights)],
            out_specs=[_pair(k, width, m) for k in range(n)],
        ),
        out_shape=[jax.ShapeDtypeStruct((rows, width), jnp.bfloat16)] * n,
        compiler_params=_params(),
        cost_estimate=_cost(2 * n * rows * sum(w.size for w in weights), weights),
    )(pos, *([t] * parts), *weights)


def _place_kernel(d_ref, *refs):
    d = d_ref[0]
    for out, u, v in zip(refs[4:], refs[:2], refs[2:4]):
        n = u.shape[1]
        out[:, pl.ds(pl.multiple_of(d * n, n), n)] = u[...]
        out[:, pl.ds(pl.multiple_of((1 - d) * n, n), n)] = v[...]


def placed(own, other, d):
    rows, n = own[0].shape
    spec = lambda w: pl.BlockSpec((BLOCK, w), lambda i, _: (i, 0))
    return pl.pallas_call(
        _place_kernel,
        grid_spec=pltpu.PrefetchScalarGridSpec(num_scalar_prefetch=1, grid=(rows // BLOCK,), in_specs=[spec(n)] * 4, out_specs=[spec(2 * n)] * 2),
        out_shape=[jax.ShapeDtypeStruct((rows, 2 * n), jnp.bfloat16)] * 2,
        compiler_params=_params(),
        cost_estimate=_cost(0, [*own, *other, *own, *other]),
    )(jnp.asarray(d, jnp.int32).reshape(1), *own, *other)


def _ffn_kernel(a_ref, b_ref, *rest, piece, m, swapped, n_back, n_given):
    back, rest = rest[:n_back], rest[n_back:]
    hbm, rest = rest[: n_back + 1], rest[n_back + 1 + n_given :]
    hid_ref, dg_ref, du_ref, lo_ref, hi_ref = rest[:5]
    dy_ref = rest[5]
    da_ref, db_ref = rest[3 + n_back + 1 : 3 + n_back + 3]
    *held, sems = rest[3 + n_back + 3 :]
    w1_ref, w2_ref = held[:2]
    k, units = w1_ref.shape[0], w1_ref.shape[1] // 2
    cuts = range(0, units, piece)

    def copies(p, at):
        for j in range(4):
            here = (slice(None), slice(at + j // 2 * units, at + j // 2 * units + piece))
            yield pltpu.make_async_copy(hbm[j % 2].at[here], held[j % 2].at[here], sems.at[5 * p + j])
        if n_back == 2:
            here = slice(at, at + piece)
            yield pltpu.make_async_copy(hbm[2].at[here], held[2].at[here], sems.at[5 * p + 4])

    @pl.when(pl.program_id(0) == 0)
    def _():
        for p, at in enumerate(cuts):
            for copy in copies(p, at):
                copy.start()

    def work(x_ref, back_ref, dx_ref, first):
        x1, x2 = x_ref[:, :k], x_ref[:, k:]
        lo_ref[...], hi_ref[...] = x1, x2
        if n_back == 2:
            dy_ref[...] = back_ref[...]
        for p, at in enumerate(cuts):
            if first:

                @pl.when(pl.program_id(0) == 0)
                def _(p=p, at=at):
                    for copy in copies(p, at):
                        copy.wait()

            here, there = slice(at, at + piece), slice(units + at, units + at + piece)
            g = _dot(x1, w1_ref[:, here], 1, 0) + _dot(x2, w2_ref[:, here], 1, 0)
            u = _dot(x1, w1_ref[:, there], 1, 0) + _dot(x2, w2_ref[:, there], 1, 0)
            dh = f32(bf16(_dot(back_ref[...], held[2][here, :], 1, 1)) if n_back == 2 else back_ref[:, here])
            s = jax.nn.sigmoid(g)
            gs = g * s
            hid_ref[:, here] = bf16(gs * u)
            dg_ref[:, here] = bf16(dh * u * (s + gs * (1 - s)))
            du_ref[:, here] = bf16(dh * gs)
        for j, w in enumerate((w2_ref, w1_ref) if swapped else (w1_ref, w2_ref)):
            dx_ref[:, j * k : (j + 1) * k] = bf16(_dot(dg_ref[...], w[:, :units], 1, 1) + _dot(du_ref[...], w[:, units:], 1, 1))

    @pl.when(pl.program_id(0) < m)
    def _():
        work(a_ref, back[0], da_ref, True)

    @pl.when(pl.program_id(0) >= m)
    def _():
        work(b_ref, back[-1], db_ref, False)


def ffn(a, b, back, weights, n, total, buffers, swapped, piece=512):
    rows, d = a.shape
    units = weights[0].shape[1] // 2
    m = rows // BLOCK
    at = lambda width: pl.BlockSpec((BLOCK, width), lambda i: (n * 2 * m + i, 0))
    anywhere = pl.BlockSpec(memory_space=pl.ANY)
    two = len(back) == 2
    backs = [_pair(0, d, m), _pair(1, d, m)] if two else [pl.BlockSpec((BLOCK, units), lambda i: (i, 0))]
    given = list(buffers or ())
    widths = (units, units, units, d // 2, d // 2) + ((d,) if two else ())
    first = 2 + len(back) + len(weights)
    *buffers, da, db = pl.pallas_call(
        functools.partial(_ffn_kernel, piece=piece, m=m, swapped=swapped, n_back=len(back), n_given=len(given)),
        grid=(2 * m,),
        in_specs=[_pair(0, d, m), _pair(1, d, m), *backs, *[anywhere] * (len(weights) + len(given))],
        out_specs=[*(at(w) for w in widths), _pair(0, d, m), _pair(1, d, m)],
        out_shape=[*(jax.ShapeDtypeStruct((total, w), jnp.bfloat16) for w in widths), *[jax.ShapeDtypeStruct((rows, d), jnp.bfloat16)] * 2],
        input_output_aliases={first + i: i for i in range(len(given))},
        scratch_shapes=[*(pltpu.VMEM(w.shape, w.dtype) for w in weights), pltpu.SemaphoreType.DMA((5 * (units // piece),))],
        compiler_params=_params(),
        cost_estimate=_cost((20 if two else 16) * rows * d * units, [a, b, *weights]),
    )(a, b, *back, *weights, *given)
    return buffers, da, db


def normed(h):
    wide = f32(h)
    scale = lax.rsqrt(jnp.mean(wide**2, -1, keepdims=True) + 1e-6)
    return bf16(wide * scale)


def normed_bwd(h, by):
    wide, by = f32(h), f32(by)
    scale = lax.rsqrt(jnp.mean(wide**2, -1, keepdims=True) + 1e-6)
    return scale * (by - wide * (scale * scale * jnp.mean(by * wide, -1, keepdims=True)))


CORE, OVER_X, OVER_Y = ("tp", ((0, 1), (1, 0), (2, 3), (3, 2))), ("tp", ((0, 2), (1, 3), (2, 0), (3, 1))), ("dp", ((0, 1), (1, 0)))


ACROSS = (("dp", "tp"), tuple((i, (i + 4) % 8 // 4 * 4 + (i + 2) % 4) for i in range(8)))


def send(way, t):
    return lax.ppermute(t, way[0], way[1])


def layer(x, dy, wq, wk, wv, wo, wg, wu, wd):
    d, t = lax.axis_index("dp"), lax.axis_index("tp")
    own, width = x.shape
    seq, units = 4 * own, wd.shape[0]
    half = width // 2
    t_core, t_x = t + 1 - 2 * lax.rem(t, 2), lax.rem(t + 2, 4)
    t_xcore = t_x + 1 - 2 * lax.rem(t, 2)
    ordered = lambda t, place: jnp.where(place == 0, t, jnp.concatenate([t[:, half:], t[:, :half]], 1))
    mine = lambda w: lax.dynamic_slice_in_dim(w, d * units, units, axis=1)
    theirs = lambda w: lax.dynamic_slice_in_dim(w, (1 - d) * units, units, axis=1)

    w_qkv = []
    for w in (wq, wk, wv):
        w_qkv += [w, send(OVER_Y, w)]
    a = ordered(normed(x), d)
    ax = send(OVER_X, a)
    ac = send(CORE, a)
    gu_send = jnp.concatenate([theirs(wg), theirs(wu)], 1)
    gu_mine = jnp.concatenate([mine(wg), mine(wu)], 1)
    wo_theirs = send(OVER_Y, wo)
    gu_theirs = send(OVER_Y, gu_send)
    axc = send(CORE, ax)

    dyc = send(CORE, dy)
    dyx = send(OVER_X, dy)
    dyxc = send(CORE, dyx)
    dyy = send(OVER_Y, dy)
    dyyc = send(CORE, dyy)
    dyd = send(OVER_X, dyy)
    dydc = send(CORE, dyd)

    angle = jnp.arange(seq, dtype=jnp.float32)[:, None] * THETA ** (-jnp.arange(HALF, dtype=jnp.float32) / HALF)
    cos, sin = jnp.cos(angle), jnp.sin(angle)

    cols = wq.shape[1]
    proj = functools.partial(rows_into, _project, weights=w_qkv, total=seq, widths=(cols, cols, cols, half, half), flops=12 * own * width * cols)
    kept = proj([a, ac], places=(t, t_core))
    *qkv, a_lo, a_hi = proj([ax, axc], places=(t_x, t_xcore), buffers=kept)
    heads, lse = attend(*qkv, cos, sin)
    o_from = functools.partial(rows_from, heads, [wo, wo_theirs], rows=own, width=width, order=d)
    ox, oxc = o_from(places=(t_x, t_xcore))
    sox = bf16(f32(ox) + f32(send(CORE, oxc)))
    o_far = send(OVER_X, sox)
    o, oc = o_from(places=(t, t_core))
    o_near = send(CORE, oc)
    h = bf16(f32(x) + f32(bf16(f32(o) + f32(o_near) + f32(o_far))))
    b = normed(h)
    b_mine, b_other = ordered(b, d), ordered(b, 1 - d)

    by = send(OVER_Y, b_other)
    bx = send(OVER_X, b_mine)
    bc = send(CORE, b_mine)
    bxc = send(CORE, bx)
    byc = send(CORE, by)
    bd = send(OVER_X, by)
    bdc = send(CORE, bd)
    dy_all, kept, sums = None, None, []
    given = ((dy, dyc, b_mine, bc), (dyx, dyxc, bx, bxc), (dyy, dyyc, by, byc), (dyd, dydc, bd, bdc))
    for n, (dy_u, dy_v, u, v) in enumerate(given):
        if n < 2:
            d_hid, dy_all = hidden_back(dy_u, dy_v, wd, n, 2 * seq, dy_all)
            back, weights = [d_hid], [gu_mine, gu_theirs]
        else:
            back, weights = [dy_u, dy_v], [gu_mine, gu_theirs, wd]
            kept = [*kept, dy_all] if n == 2 else kept
        kept, du, dv = ffn(u, v, back, weights, n, 2 * seq, kept, n >= 2)
        near = send(CORE, dv)
        total = f32(du) + f32(near)
        sums.append(bf16(total) if n else total)
    hid, dg, du, b_lo, b_hi, dy_all = kept
    from_x = send(OVER_X, sums[1])
    from_y = send(OVER_Y, sums[2])
    from_d = send(ACROSS, sums[3])
    db = bf16(ordered(sums[0] + f32(from_x) + f32(from_y) + f32(from_d), d))
    dh = bf16(f32(dy) + f32(bf16(normed_bwd(h, db))))

    got_gu, kept_gu = [], []
    for g in (dg, du):
        part = bf16(_dot(b_hi, g, 0, 0))
        got_gu.append(send(OVER_Y, part))
        kept_gu.append(bf16(_dot(b_lo, g, 0, 0)))
    d_wd = bf16(_dot(hid, dy_all, 0, 0))

    dhx = send(OVER_X, dh)
    dhc = send(CORE, dh)
    dhxc = send(CORE, dhx)
    heads_back = functools.partial(rows_into, _heads_back, weights=(wo, wo_theirs), total=seq, widths=(heads.shape[1], width), flops=8 * own * width * heads.shape[1])
    d_heads, dh_all = heads_back([dh, dhc, dhx, dhxc], places=(t, t_core, t_x, t_xcore, d))
    d_qkv = attend_bwd(*qkv, d_heads, lse, cos, sin)
    part = bf16(_dot(a_hi, d_qkv, 0, 0))
    got = send(OVER_Y, part)
    dax, daxc, da, dac = rows_from(d_qkv, w_qkv, (t_x, t_xcore, t, t_core), own, width)
    sdax = bf16(f32(dax) + f32(send(CORE, daxc)))
    da_far = send(OVER_X, sdax)
    da_near = send(CORE, dac)
    d_wo_all = bf16(_dot(heads, dh_all, 0, 0))
    rows = wo.shape[0]
    wo_part = lambda i: lax.dynamic_slice_in_dim(d_wo_all, i * rows, rows, axis=0)
    wo_send = wo_part(1 - d)
    wo_got = send(OVER_Y, wo_send)
    part_kept = lax.optimization_barrier(_dot(a_lo, d_qkv, 0, 0))
    d_wg, d_wu = placed(kept_gu, got_gu, d)
    da_sum = bf16(ordered(f32(da) + f32(da_near) + f32(da_far), d))
    dx = bf16(f32(dh) + f32(bf16(normed_bwd(x, da_sum))))
    d_w_qkv = [bf16(part_kept[:, i : i + cols] + f32(got[:, i : i + cols])) for i in range(0, 3 * cols, cols)]
    d_wo = bf16(f32(wo_part(d)) + f32(wo_got))
    return dx, *d_w_qkv, d_wo, d_wg, d_wu, d_wd


def solution(mesh):
    def step(x, dy, *weights):
        dx, *rest = layer(x[0], dy[0], *weights)
        return (dx[None], *rest)

    states, by_columns, by_rows = P("dp", "tp", None), P("dp", "tp"), P(("tp", "dp"), None)
    weights = (by_columns, by_columns, by_columns, by_rows, by_columns, by_columns, by_rows)
    return jax.shard_map(step, mesh=mesh, in_specs=(states, states, *weights), out_specs=(states, *weights), check_vma=False)
```

```python
import functools

import jax
import jax.numpy as jnp
from jax import lax
from jax.experimental import pallas as pl
from jax.experimental.pallas import tpu as pltpu
from jax.sharding import PartitionSpec as P

HEAD = 256
HALF = HEAD // 2
THETA = 10000
LOG2E = 1.4426950408889634
HIDDEN = -1e30
VMEM = 58 * 2**20


def _dot(a, b, ca, cb):
    return lax.dot_general(a, b, (((ca,), (cb,)), ((), ())), preferred_element_type=jnp.float32)


def _turn(t, cos, sin):
    a, b = t[:, :HALF].astype(jnp.float32), t[:, HALF:].astype(jnp.float32)
    return jnp.concatenate([a * cos - b * sin, b * cos + a * sin], -1).astype(jnp.bfloat16)


def _turn_back(t, cos, sin):
    a, b = t[:, :HALF], t[:, HALF:]
    return jnp.concatenate([a * cos + b * sin, b * cos - a * sin], -1).astype(jnp.bfloat16)


def _mask(n):
    return lax.broadcasted_iota(jnp.int32, (n, n), 1) >= lax.broadcasted_iota(jnp.int32, (n, n), 0)


def _fwd_kernel(q_ref, k_ref, v_ref, cos_ref, sin_ref, o_ref, lse_ref, k_s, *, strip):
    tokens = q_ref.shape[0]
    e = HEAD**-0.5 * LOG2E
    ok = _mask(strip)
    for i in range(tokens // strip):
        here = pl.ds(i * strip, strip)
        cos, sin = cos_ref[here, :], sin_ref[here, :]
        q = _turn(q_ref[here, :], cos, sin)
        k_s[here, :] = _turn(k_ref[here, :], cos, sin)
        n = i * strip
        diag = jnp.where(ok, _dot(k_s[here, :], q, 1, 1), HIDDEN)
        top = diag.max(axis=0, keepdims=True)
        if n:
            past = _dot(k_s[:n, :], q, 1, 1)
            top = jnp.maximum(top, past.max(axis=0, keepdims=True))
        p = jnp.exp2((diag - top) * e)
        total = p.sum(axis=0, keepdims=True)
        out = _dot(v_ref[here, :], p.astype(jnp.bfloat16), 0, 0)
        if n:
            p = jnp.exp2((past - top) * e)
            total += p.sum(axis=0, keepdims=True)
            out += _dot(v_ref[:n, :], p.astype(jnp.bfloat16), 0, 0)
        o_ref[here, :] = (out * (1 / total)).T.astype(jnp.bfloat16)
        lse_ref[0, :, here] = top * e + jnp.log2(total)


def attend(q, k, v, cos, sin, strip=512):
    tokens, heads = q.shape[0], q.shape[1] // HEAD
    column = pl.BlockSpec((tokens, HEAD), lambda h: (0, h))
    whole = pl.BlockSpec((tokens, HALF), lambda h: (0, 0))
    return pl.pallas_call(
        functools.partial(_fwd_kernel, strip=strip),
        grid=(heads,),
        in_specs=[column, column, column, whole, whole],
        out_specs=[column, pl.BlockSpec((1, 1, tokens), lambda h: (h, 0, 0))],
        out_shape=[jax.ShapeDtypeStruct((tokens, heads * HEAD), jnp.bfloat16), jax.ShapeDtypeStruct((heads, 1, tokens), jnp.float32)],
        scratch_shapes=[pltpu.VMEM((tokens, HEAD), jnp.bfloat16)],
        compiler_params=pltpu.CompilerParams(dimension_semantics=("arbitrary",), vmem_limit_bytes=VMEM),
        cost_estimate=pl.CostEstimate(flops=4 * heads * tokens * tokens * HEAD, transcendentals=heads * tokens * tokens, bytes_accessed=4 * tokens * heads * HEAD * 2),
    )(q, k, v, cos, sin)


def _bwd_kernel(q_ref, k_ref, v_ref, do_ref, lse_ref, cos_ref, sin_ref, out_ref, k_s, dk_s, dv_s, *, strip):
    tokens = q_ref.shape[0]
    scale = HEAD**-0.5
    e = scale * LOG2E

    def put(j, rows, t):
        at = (j * pl.num_programs(0) + pl.program_id(0)) * HEAD
        out_ref[rows, pl.ds(pl.multiple_of(at, HEAD), HEAD)] = t

    ok = _mask(strip)
    for i in range(tokens // strip):
        here = pl.ds(i * strip, strip)
        cos, sin = cos_ref[here, :], sin_ref[here, :]
        q = _turn(q_ref[here, :], cos, sin)
        k_s[here, :] = _turn(k_ref[here, :], cos, sin)
        do, lse = do_ref[here, :], lse_ref[0, :, here]
        n = i * strip
        p = jnp.where(ok, jnp.exp2(_dot(k_s[here, :], q, 1, 1) * e - lse), 0.0)
        dp = _dot(v_ref[here, :], do, 1, 1)
        delta = (p * dp).sum(axis=0, keepdims=True)
        if n:
            p0 = jnp.exp2(_dot(k_s[:n, :], q, 1, 1) * e - lse)
            dp0 = _dot(v_ref[:n, :], do, 1, 1)
            delta += (p0 * dp0).sum(axis=0, keepdims=True)
        ds = (p * (dp - delta)).astype(jnp.bfloat16)
        dv_s[here, :] = _dot(p.astype(jnp.bfloat16), do, 1, 0)
        dk_s[here, :] = _dot(ds, q, 1, 0)
        dq = _dot(ds, k_s[here, :], 0, 0)
        if n:
            ds0 = (p0 * (dp0 - delta)).astype(jnp.bfloat16)
            dv_s[:n, :] += _dot(p0.astype(jnp.bfloat16), do, 1, 0)
            dk_s[:n, :] += _dot(ds0, q, 1, 0)
            dq += _dot(ds0, k_s[:n, :], 0, 0)
        put(0, here, _turn_back(dq * scale, cos, sin))
    for i in range(tokens // strip):
        here = pl.ds(i * strip, strip)
        put(1, here, _turn_back(dk_s[here, :] * scale, cos_ref[here, :], sin_ref[here, :]))
        put(2, here, dv_s[here, :].astype(jnp.bfloat16))


def attend_bwd(q, k, v, d_out, lse, cos, sin, strip=512):
    tokens, heads = q.shape[0], q.shape[1] // HEAD
    column = pl.BlockSpec((tokens, HEAD), lambda h: (0, h))
    whole = pl.BlockSpec((tokens, HALF), lambda h: (0, 0))
    return pl.pallas_call(
        functools.partial(_bwd_kernel, strip=strip),
        grid=(heads,),
        in_specs=[column, column, column, column, pl.BlockSpec((1, 1, tokens), lambda h: (h, 0, 0)), whole, whole],
        out_specs=pl.BlockSpec((tokens, 3 * heads * HEAD), lambda h: (0, 0), pipeline_mode=pl.Buffered(1)),
        out_shape=jax.ShapeDtypeStruct((tokens, 3 * heads * HEAD), jnp.bfloat16),
        scratch_shapes=[pltpu.VMEM((tokens, HEAD), jnp.bfloat16), pltpu.VMEM((tokens, HEAD), jnp.float32), pltpu.VMEM((tokens, HEAD), jnp.float32)],
        compiler_params=pltpu.CompilerParams(dimension_semantics=("arbitrary",), vmem_limit_bytes=VMEM),
        cost_estimate=pl.CostEstimate(flops=10 * heads * tokens * tokens * HEAD, transcendentals=heads * tokens * tokens, bytes_accessed=7 * tokens * heads * HEAD * 2),
    )(q, k, v, d_out, lse, cos, sin)


BLOCK = 256


def _params(n=1):
    return pltpu.CompilerParams(dimension_semantics=("arbitrary",) * n, vmem_limit_bytes=VMEM)


def _pair(k, n, m):
    return pl.BlockSpec((BLOCK, n), lambda i, *_: (jnp.clip(i - k * m, 0, m - 1), 0))


def _kept(shape):
    return pl.BlockSpec(shape, lambda i, *_: (0, 0), pipeline_mode=pl.Buffered(1))


def _cost(flops, arrays):
    return pl.CostEstimate(flops=flops, transcendentals=0, bytes_accessed=sum(a.size * a.dtype.itemsize for a in arrays))


def _rows_kernel(pos_ref, *refs, work, m, n_in, n_w, n_out):
    for k in range(n_in):

        @pl.when(pl.program_id(0) // m == k)
        def _(k=k):
            work(refs[k], refs[n_in : n_in + n_w], refs[-n_out:], pos_ref)


def rows_into(work, arrays, weights, places, total, widths, buffers=None, flops=0):
    rows, n_in = arrays[0].shape[0], len(arrays)
    m = rows // BLOCK
    pos = jnp.stack([jnp.asarray(p, jnp.int32) for p in places])
    out = lambda n: pl.BlockSpec((BLOCK, n), lambda i, pos: (pos[i // m] * m + i % m, 0))
    given = list(buffers or ())
    return pl.pallas_call(
        functools.partial(_rows_kernel, work=work, m=m, n_in=n_in, n_w=len(weights), n_out=len(widths)),
        grid_spec=pltpu.PrefetchScalarGridSpec(
            num_scalar_prefetch=1,
            grid=(n_in * m,),
            in_specs=[*(_pair(k, a.shape[1], m) for k, a in enumerate(arrays)), *(_kept(w.shape) for w in weights), *(pl.BlockSpec(memory_space=pl.ANY) for _ in given)],
            out_specs=[out(n) for n in widths],
        ),
        out_shape=[jax.ShapeDtypeStruct((total, n), jnp.bfloat16) for n in widths],
        input_output_aliases={1 + n_in + len(weights) + i: i for i in range(len(given))},
        compiler_params=_params(),
        cost_estimate=_cost(flops, [*arrays, *weights]),
    )(pos, *arrays, *weights, *given)


def bf16(t):
    return t.astype(jnp.bfloat16)


def f32(t):
    return t.astype(jnp.float32)


def _project(a_ref, w_refs, outs, pos_ref):
    k = w_refs[0].shape[0]
    for out, first, second in zip(outs, w_refs[::2], w_refs[1::2]):
        out[...] = bf16(_dot(a_ref[:, :k], first[...], 1, 0) + _dot(a_ref[:, k:], second[...], 1, 0))
    outs[-2][...], outs[-1][...] = a_ref[:, :k], a_ref[:, k:]


def _hidden_back_kernel(a_ref, b_ref, w_ref, *rest, m):
    out_ref, copy_ref = rest[-2:]

    def work(x_ref):
        out_ref[...] = bf16(_dot(x_ref[...], w_ref[...], 1, 1))
        copy_ref[...] = x_ref[...]

    @pl.when(pl.program_id(0) < m)
    def _():
        work(a_ref)

    @pl.when(pl.program_id(0) >= m)
    def _():
        work(b_ref)


def hidden_back(a, b, w, n, total, buffer):
    rows, d = a.shape
    m = rows // BLOCK
    given = [] if buffer is None else [buffer]
    return pl.pallas_call(
        functools.partial(_hidden_back_kernel, m=m),
        grid=(2 * m,),
        in_specs=[_pair(0, d, m), _pair(1, d, m), _kept(w.shape), *(pl.BlockSpec(memory_space=pl.ANY) for _ in given)],
        out_specs=[pl.BlockSpec((BLOCK, w.shape[0]), lambda i: (i, 0)), pl.BlockSpec((BLOCK, d), lambda i: (n * 2 * m + i, 0))],
        out_shape=[jax.ShapeDtypeStruct((2 * rows, w.shape[0]), jnp.bfloat16), jax.ShapeDtypeStruct((total, d), jnp.bfloat16)],
        input_output_aliases={3: 1} if given else {},
        compiler_params=_params(),
        cost_estimate=_cost(4 * rows * d * w.shape[0], [a, b, w]),
    )(a, b, w, *given)


def _heads_back(a_ref, w_refs, outs, pos_ref):
    a = a_ref[...]
    n = w_refs[0].shape[0]
    for j, w in enumerate(w_refs):
        place = pos_ref[4] if j == 0 else 1 - pos_ref[4]
        outs[0][:, pl.ds(pl.multiple_of(place * n, n), n)] = bf16(_dot(a, w[...], 1, 1))
    outs[1][...] = a


def _from_kernel(pos_ref, *refs, turned, n_in, n_w):
    ins, w_refs, outs = refs[:n_in], refs[n_in : n_in + n_w], refs[n_in + n_w :]

    def put(o_ref):
        if turned:
            n = w_refs[0].shape[0]
            for j in range(2):
                o_ref[:, j * n : (j + 1) * n] = bf16(sum(_dot(a[...], w[...], 1, 1) for a, w in zip(ins, w_refs[j::2])))
        else:
            o_ref[...] = bf16(sum(_dot(a[...], w[...], 1, 0) for a, w in zip(ins, w_refs)))

    m = pl.num_programs(0) // len(outs)
    for k, o_ref in enumerate(outs):

        @pl.when(pl.program_id(0) // m == k)
        def _(o_ref=o_ref):
            put(o_ref)


def rows_from(t, weights, places, rows, width, order=None):
    m, n = rows // BLOCK, len(places)
    turned = order is None
    pos = jnp.stack([jnp.asarray(p, jnp.int32) for p in (*places, 0 if turned else order)])
    parts = len(weights) // 2 if turned else 2
    wide = t.shape[1] // parts
    column = lambda j, pos: j if turned else pos[n] if j == 0 else 1 - pos[n]
    ins = [pl.BlockSpec((BLOCK, wide), lambda i, pos, j=j: (pos[i // m] * m + i % m, column(j, pos))) for j in range(parts)]
    return pl.pallas_call(
        functools.partial(_from_kernel, turned=turned, n_in=parts, n_w=len(weights)),
        grid_spec=pltpu.PrefetchScalarGridSpec(
            num_scalar_prefetch=1,
            grid=(n * m,),
            in_specs=[*ins, *(_kept(w.shape) for w in weights)],
            out_specs=[_pair(k, width, m) for k in range(n)],
        ),
        out_shape=[jax.ShapeDtypeStruct((rows, width), jnp.bfloat16)] * n,
        compiler_params=_params(),
        cost_estimate=_cost(2 * n * rows * sum(w.size for w in weights), weights),
    )(pos, *([t] * parts), *weights)


def _place_kernel(d_ref, *refs):
    d = d_ref[0]
    for out, u, v in zip(refs[4:], refs[:2], refs[2:4]):
        n = u.shape[1]
        out[:, pl.ds(pl.multiple_of(d * n, n), n)] = u[...]
        out[:, pl.ds(pl.multiple_of((1 - d) * n, n), n)] = v[...]


def placed(own, other, d):
    rows, n = own[0].shape
    spec = lambda w: pl.BlockSpec((BLOCK, w), lambda i, _: (i, 0))
    return pl.pallas_call(
        _place_kernel,
        grid_spec=pltpu.PrefetchScalarGridSpec(num_scalar_prefetch=1, grid=(rows // BLOCK,), in_specs=[spec(n)] * 4, out_specs=[spec(2 * n)] * 2),
        out_shape=[jax.ShapeDtypeStruct((rows, 2 * n), jnp.bfloat16)] * 2,
        compiler_params=_params(),
        cost_estimate=_cost(0, [*own, *other, *own, *other]),
    )(jnp.asarray(d, jnp.int32).reshape(1), *own, *other)


def _ffn_kernel(a_ref, b_ref, *rest, piece, m, swapped, n_back, n_given):
    back, rest = rest[:n_back], rest[n_back:]
    hbm, rest = rest[: n_back + 1], rest[n_back + 1 + n_given :]
    hid_ref, dg_ref, du_ref, lo_ref, hi_ref = rest[:5]
    dy_ref = rest[5]
    da_ref, db_ref = rest[3 + n_back + 1 : 3 + n_back + 3]
    *held, sems = rest[3 + n_back + 3 :]
    w1_ref, w2_ref = held[:2]
    k, units = w1_ref.shape[0], w1_ref.shape[1] // 2
    cuts = range(0, units, piece)

    def copies(p, at):
        for j in range(4):
            here = (slice(None), slice(at + j // 2 * units, at + j // 2 * units + piece))
            yield pltpu.make_async_copy(hbm[j % 2].at[here], held[j % 2].at[here], sems.at[5 * p + j])
        if n_back == 2:
            here = slice(at, at + piece)
            yield pltpu.make_async_copy(hbm[2].at[here], held[2].at[here], sems.at[5 * p + 4])

    def work(x_ref, back_ref, dx_ref, first):
        x1, x2 = x_ref[:, :k], x_ref[:, k:]
        lo_ref[...], hi_ref[...] = x1, x2
        if n_back == 2:
            dy_ref[...] = back_ref[...]
        for p, at in enumerate(cuts):
            if first:
                for copy in copies(p, at):
                    copy.wait()
            here, there = slice(at, at + piece), slice(units + at, units + at + piece)
            g = _dot(x1, w1_ref[:, here], 1, 0) + _dot(x2, w2_ref[:, here], 1, 0)
            u = _dot(x1, w1_ref[:, there], 1, 0) + _dot(x2, w2_ref[:, there], 1, 0)
            dh = f32(bf16(_dot(back_ref[...], held[2][here, :], 1, 1)) if n_back == 2 else back_ref[:, here])
            s = jax.nn.sigmoid(g)
            gs = g * s
            hid_ref[:, here] = bf16(gs * u)
            dg_ref[:, here] = bf16(dh * u * (s + gs * (1 - s)))
            du_ref[:, here] = bf16(dh * gs)
        for j, w in enumerate((w2_ref, w1_ref) if swapped else (w1_ref, w2_ref)):
            dx_ref[:, j * k : (j + 1) * k] = bf16(_dot(dg_ref[...], w[:, :units], 1, 1) + _dot(du_ref[...], w[:, units:], 1, 1))

    @pl.when(pl.program_id(0) == 0)
    def _():
        for p, at in enumerate(cuts):
            for copy in copies(p, at):
                copy.start()
        work(a_ref, back[0], da_ref, True)

    @pl.when((pl.program_id(0) > 0) & (pl.program_id(0) < m))
    def _():
        work(a_ref, back[0], da_ref, False)

    @pl.when(pl.program_id(0) >= m)
    def _():
        work(b_ref, back[-1], db_ref, False)


def ffn(a, b, back, weights, n, total, buffers, swapped, piece=768):
    rows, d = a.shape
    units = weights[0].shape[1] // 2
    m = rows // BLOCK
    at = lambda width: pl.BlockSpec((BLOCK, width), lambda i: (n * 2 * m + i, 0))
    anywhere = pl.BlockSpec(memory_space=pl.ANY)
    two = len(back) == 2
    backs = [_pair(0, d, m), _pair(1, d, m)] if two else [pl.BlockSpec((BLOCK, units), lambda i: (i, 0))]
    given = list(buffers or ())
    widths = (units, units, units, d // 2, d // 2) + ((d,) if two else ())
    first = 2 + len(back) + len(weights)
    *buffers, da, db = pl.pallas_call(
        functools.partial(_ffn_kernel, piece=piece, m=m, swapped=swapped, n_back=len(back), n_given=len(given)),
        grid=(2 * m,),
        in_specs=[_pair(0, d, m), _pair(1, d, m), *backs, *[anywhere] * (len(weights) + len(given))],
        out_specs=[*(at(w) for w in widths), _pair(0, d, m), _pair(1, d, m)],
        out_shape=[*(jax.ShapeDtypeStruct((total, w), jnp.bfloat16) for w in widths), *[jax.ShapeDtypeStruct((rows, d), jnp.bfloat16)] * 2],
        input_output_aliases={first + i: i for i in range(len(given))},
        scratch_shapes=[*(pltpu.VMEM(w.shape, w.dtype) for w in weights), pltpu.SemaphoreType.DMA((5 * (units // piece),))],
        compiler_params=_params(),
        cost_estimate=_cost((20 if two else 16) * rows * d * units, [a, b, *weights]),
    )(a, b, *back, *weights, *given)
    return buffers, da, db


def normed(h):
    wide = f32(h)
    scale = lax.rsqrt(jnp.mean(wide**2, -1, keepdims=True) + 1e-6)
    return bf16(wide * scale)


def normed_bwd(h, by):
    wide, by = f32(h), f32(by)
    scale = lax.rsqrt(jnp.mean(wide**2, -1, keepdims=True) + 1e-6)
    return scale * (by - wide * (scale * scale * jnp.mean(by * wide, -1, keepdims=True)))


CORE, OVER_X, OVER_Y = ("tp", ((0, 1), (1, 0), (2, 3), (3, 2))), ("tp", ((0, 2), (1, 3), (2, 0), (3, 1))), ("dp", ((0, 1), (1, 0)))


ACROSS = (("dp", "tp"), tuple((i, (i + 4) % 8 // 4 * 4 + (i + 2) % 4) for i in range(8)))


def send(way, t):
    return lax.ppermute(t, way[0], way[1])


def layer(x, dy, wq, wk, wv, wo, wg, wu, wd):
    d, t = lax.axis_index("dp"), lax.axis_index("tp")
    own, width = x.shape
    seq, units = 4 * own, wd.shape[0]
    half = width // 2
    t_core, t_x = t + 1 - 2 * lax.rem(t, 2), lax.rem(t + 2, 4)
    t_xcore = t_x + 1 - 2 * lax.rem(t, 2)
    ordered = lambda t, place: jnp.where(place == 0, t, jnp.concatenate([t[:, half:], t[:, :half]], 1))
    mine = lambda w: lax.dynamic_slice_in_dim(w, d * units, units, axis=1)
    theirs = lambda w: lax.dynamic_slice_in_dim(w, (1 - d) * units, units, axis=1)

    w_qkv = []
    for w in (wq, wk, wv):
        w_qkv += [w, send(OVER_Y, w)]
    a = ordered(normed(x), d)
    ax = send(OVER_X, a)
    ac = send(CORE, a)
    gu_send = jnp.concatenate([theirs(wg), theirs(wu)], 1)
    gu_mine = jnp.concatenate([mine(wg), mine(wu)], 1)
    wo_theirs = send(OVER_Y, wo)
    gu_theirs = send(OVER_Y, gu_send)
    axc = send(CORE, ax)

    dyc = send(CORE, dy)
    dyx = send(OVER_X, dy)
    dyxc = send(CORE, dyx)
    dyy = send(OVER_Y, dy)
    dyyc = send(CORE, dyy)
    dyd = send(OVER_X, dyy)
    dydc = send(CORE, dyd)

    angle = jnp.arange(seq, dtype=jnp.float32)[:, None] * THETA ** (-jnp.arange(HALF, dtype=jnp.float32) / HALF)
    cos, sin = jnp.cos(angle), jnp.sin(angle)

    cols = wq.shape[1]
    proj = functools.partial(rows_into, _project, weights=w_qkv, total=seq, widths=(cols, cols, cols, half, half), flops=12 * own * width * cols)
    kept = proj([a, ac], places=(t, t_core))
    *qkv, a_lo, a_hi = proj([ax, axc], places=(t_x, t_xcore), buffers=kept)
    heads, lse = attend(*qkv, cos, sin)
    o_from = functools.partial(rows_from, heads, [wo, wo_theirs], rows=own, width=width, order=d)
    ox, oxc = o_from(places=(t_x, t_xcore))
    sox = bf16(f32(ox) + f32(send(CORE, oxc)))
    o_far = send(OVER_X, sox)
    o, oc = o_from(places=(t, t_core))
    o_near = send(CORE, oc)
    h = bf16(f32(x) + f32(bf16(f32(o) + f32(o_near) + f32(o_far))))
    b = normed(h)
    b_mine, b_other = ordered(b, d), ordered(b, 1 - d)

    by = send(OVER_Y, b_other)
    bx = send(OVER_X, b_mine)
    bc = send(CORE, b_mine)
    bxc = send(CORE, bx)
    byc = send(CORE, by)
    bd = send(OVER_X, by)
    bdc = send(CORE, bd)
    dy_all, kept, sums = None, None, []
    given = ((dy, dyc, b_mine, bc), (dyx, dyxc, bx, bxc), (dyy, dyyc, by, byc), (dyd, dydc, bd, bdc))
    for n, (dy_u, dy_v, u, v) in enumerate(given):
        if n < 2:
            d_hid, dy_all = hidden_back(dy_u, dy_v, wd, n, 2 * seq, dy_all)
            back, weights = [d_hid], [gu_mine, gu_theirs]
        else:
            back, weights = [dy_u, dy_v], [gu_mine, gu_theirs, wd]
            kept = [*kept, dy_all] if n == 2 else kept
        kept, du, dv = ffn(u, v, back, weights, n, 2 * seq, kept, n >= 2)
        near = send(CORE, dv)
        total = f32(du) + f32(near)
        sums.append(bf16(total) if n else total)
    hid, dg, du, b_lo, b_hi, dy_all = kept
    from_x = send(OVER_X, sums[1])
    from_y = send(OVER_Y, sums[2])
    from_d = send(ACROSS, sums[3])
    db = bf16(ordered(sums[0] + f32(from_x) + f32(from_y) + f32(from_d), d))
    dh = bf16(f32(dy) + f32(bf16(normed_bwd(h, db))))

    got_gu, kept_gu = [], []
    for g in (dg, du):
        part = bf16(_dot(b_hi, g, 0, 0))
        got_gu.append(send(OVER_Y, part))
        kept_gu.append(bf16(_dot(b_lo, g, 0, 0)))
    d_wd = bf16(_dot(hid, dy_all, 0, 0))

    dhx = send(OVER_X, dh)
    dhc = send(CORE, dh)
    dhxc = send(CORE, dhx)
    heads_back = functools.partial(rows_into, _heads_back, weights=(wo, wo_theirs), total=seq, widths=(heads.shape[1], width), flops=8 * own * width * heads.shape[1])
    d_heads, dh_all = heads_back([dh, dhc, dhx, dhxc], places=(t, t_core, t_x, t_xcore, d))
    d_qkv = attend_bwd(*qkv, d_heads, lse, cos, sin)
    part = bf16(_dot(a_hi, d_qkv, 0, 0))
    got = send(OVER_Y, part)
    dax, daxc, da, dac = rows_from(d_qkv, w_qkv, (t_x, t_xcore, t, t_core), own, width)
    sdax = bf16(f32(dax) + f32(send(CORE, daxc)))
    da_far = send(OVER_X, sdax)
    da_near = send(CORE, dac)
    d_wo_all = bf16(_dot(heads, dh_all, 0, 0))
    rows = wo.shape[0]
    wo_part = lambda i: lax.dynamic_slice_in_dim(d_wo_all, i * rows, rows, axis=0)
    wo_send = wo_part(1 - d)
    wo_got = send(OVER_Y, wo_send)
    part_kept = lax.optimization_barrier(_dot(a_lo, d_qkv, 0, 0))
    d_wg, d_wu = placed(kept_gu, got_gu, d)
    da_sum = bf16(ordered(f32(da) + f32(da_near) + f32(da_far), d))
    dx = bf16(f32(dh) + f32(bf16(normed_bwd(x, da_sum))))
    d_w_qkv = [bf16(part_kept[:, i : i + cols] + f32(got[:, i : i + cols])) for i in range(0, 3 * cols, cols)]
    d_wo = bf16(f32(wo_part(d)) + f32(wo_got))
    return dx, *d_w_qkv, d_wo, d_wg, d_wu, d_wd


def solution(mesh):
    def step(x, dy, *weights):
        dx, *rest = layer(x[0], dy[0], *weights)
        return (dx[None], *rest)

    states, by_columns, by_rows = P("dp", "tp", None), P("dp", "tp"), P(("tp", "dp"), None)
    weights = (by_columns, by_columns, by_columns, by_rows, by_columns, by_columns, by_rows)
    return jax.shard_map(step, mesh=mesh, in_specs=(states, states, *weights), out_specs=(states, *weights), check_vma=False)
```

```python
import functools

import jax
import jax.numpy as jnp
from jax import lax
from jax.experimental import pallas as pl
from jax.experimental.pallas import tpu as pltpu
from jax.sharding import PartitionSpec as P

HEAD = 256
HALF = HEAD // 2
THETA = 10000
LOG2E = 1.4426950408889634
HIDDEN = -1e30
VMEM = 58 * 2**20


def _dot(a, b, ca, cb):
    return lax.dot_general(a, b, (((ca,), (cb,)), ((), ())), preferred_element_type=jnp.float32)


def _turn(t, cos, sin):
    a, b = t[:, :HALF].astype(jnp.float32), t[:, HALF:].astype(jnp.float32)
    return jnp.concatenate([a * cos - b * sin, b * cos + a * sin], -1).astype(jnp.bfloat16)


def _turn_back(t, cos, sin):
    a, b = t[:, :HALF], t[:, HALF:]
    return jnp.concatenate([a * cos + b * sin, b * cos - a * sin], -1).astype(jnp.bfloat16)


def _mask(n):
    return lax.broadcasted_iota(jnp.int32, (n, n), 1) >= lax.broadcasted_iota(jnp.int32, (n, n), 0)


def _fwd_kernel(q_ref, k_ref, v_ref, cos_ref, sin_ref, o_ref, lse_ref, k_s, *, strip):
    tokens = q_ref.shape[0]
    e = HEAD**-0.5 * LOG2E
    ok = _mask(strip)
    for i in range(tokens // strip):
        here = pl.ds(i * strip, strip)
        cos, sin = cos_ref[here, :], sin_ref[here, :]
        q = _turn(q_ref[here, :], cos, sin)
        k_s[here, :] = _turn(k_ref[here, :], cos, sin)
        n = i * strip
        diag = jnp.where(ok, _dot(k_s[here, :], q, 1, 1), HIDDEN)
        top = diag.max(axis=0, keepdims=True)
        if n:
            past = _dot(k_s[:n, :], q, 1, 1)
            top = jnp.maximum(top, past.max(axis=0, keepdims=True))
        p = jnp.exp2((diag - top) * e)
        total = p.sum(axis=0, keepdims=True)
        out = _dot(v_ref[here, :], p.astype(jnp.bfloat16), 0, 0)
        if n:
            p = jnp.exp2((past - top) * e)
            total += p.sum(axis=0, keepdims=True)
            out += _dot(v_ref[:n, :], p.astype(jnp.bfloat16), 0, 0)
        o_ref[here, :] = (out * (1 / total)).T.astype(jnp.bfloat16)
        lse_ref[0, :, here] = top * e + jnp.log2(total)


def attend(q, k, v, cos, sin, strip=512):
    tokens, heads = q.shape[0], q.shape[1] // HEAD
    column = pl.BlockSpec((tokens, HEAD), lambda h: (0, h))
    whole = pl.BlockSpec((tokens, HALF), lambda h: (0, 0))
    return pl.pallas_call(
        functools.partial(_fwd_kernel, strip=strip),
        grid=(heads,),
        in_specs=[column, column, column, whole, whole],
        out_specs=[column, pl.BlockSpec((1, 1, tokens), lambda h: (h, 0, 0))],
        out_shape=[jax.ShapeDtypeStruct((tokens, heads * HEAD), jnp.bfloat16), jax.ShapeDtypeStruct((heads, 1, tokens), jnp.float32)],
        scratch_shapes=[pltpu.VMEM((tokens, HEAD), jnp.bfloat16)],
        compiler_params=pltpu.CompilerParams(dimension_semantics=("arbitrary",), vmem_limit_bytes=VMEM),
        cost_estimate=pl.CostEstimate(flops=4 * heads * tokens * tokens * HEAD, transcendentals=heads * tokens * tokens, bytes_accessed=4 * tokens * heads * HEAD * 2),
    )(q, k, v, cos, sin)


def _bwd_kernel(q_ref, k_ref, v_ref, do_ref, lse_ref, cos_ref, sin_ref, out_ref, k_s, dk_s, dv_s, *, strip):
    tokens = q_ref.shape[0]
    scale = HEAD**-0.5
    e = scale * LOG2E

    def put(j, rows, t):
        at = (j * pl.num_programs(0) + pl.program_id(0)) * HEAD
        out_ref[rows, pl.ds(pl.multiple_of(at, HEAD), HEAD)] = t

    ok = _mask(strip)
    for i in range(tokens // strip):
        here = pl.ds(i * strip, strip)
        cos, sin = cos_ref[here, :], sin_ref[here, :]
        q = _turn(q_ref[here, :], cos, sin)
        k_s[here, :] = _turn(k_ref[here, :], cos, sin)
        do, lse = do_ref[here, :], lse_ref[0, :, here]
        n = i * strip
        p = jnp.where(ok, jnp.exp2(_dot(k_s[here, :], q, 1, 1) * e - lse), 0.0)
        dp = _dot(v_ref[here, :], do, 1, 1)
        delta = (p * dp).sum(axis=0, keepdims=True)
        if n:
            p0 = jnp.exp2(_dot(k_s[:n, :], q, 1, 1) * e - lse)
            dp0 = _dot(v_ref[:n, :], do, 1, 1)
            delta += (p0 * dp0).sum(axis=0, keepdims=True)
        ds = (p * (dp - delta)).astype(jnp.bfloat16)
        dv_s[here, :] = _dot(p.astype(jnp.bfloat16), do, 1, 0)
        dk_s[here, :] = _dot(ds, q, 1, 0)
        dq = _dot(ds, k_s[here, :], 0, 0)
        if n:
            ds0 = (p0 * (dp0 - delta)).astype(jnp.bfloat16)
            dv_s[:n, :] += _dot(p0.astype(jnp.bfloat16), do, 1, 0)
            dk_s[:n, :] += _dot(ds0, q, 1, 0)
            dq += _dot(ds0, k_s[:n, :], 0, 0)
        put(0, here, _turn_back(dq * scale, cos, sin))
    for i in range(tokens // strip):
        here = pl.ds(i * strip, strip)
        put(1, here, _turn_back(dk_s[here, :] * scale, cos_ref[here, :], sin_ref[here, :]))
        put(2, here, dv_s[here, :].astype(jnp.bfloat16))


def attend_bwd(q, k, v, d_out, lse, cos, sin, strip=512):
    tokens, heads = q.shape[0], q.shape[1] // HEAD
    column = pl.BlockSpec((tokens, HEAD), lambda h: (0, h))
    whole = pl.BlockSpec((tokens, HALF), lambda h: (0, 0))
    return pl.pallas_call(
        functools.partial(_bwd_kernel, strip=strip),
        grid=(heads,),
        in_specs=[column, column, column, column, pl.BlockSpec((1, 1, tokens), lambda h: (h, 0, 0)), whole, whole],
        out_specs=pl.BlockSpec((tokens, 3 * heads * HEAD), lambda h: (0, 0), pipeline_mode=pl.Buffered(1)),
        out_shape=jax.ShapeDtypeStruct((tokens, 3 * heads * HEAD), jnp.bfloat16),
        scratch_shapes=[pltpu.VMEM((tokens, HEAD), jnp.bfloat16), pltpu.VMEM((tokens, HEAD), jnp.float32), pltpu.VMEM((tokens, HEAD), jnp.float32)],
        compiler_params=pltpu.CompilerParams(dimension_semantics=("arbitrary",), vmem_limit_bytes=VMEM),
        cost_estimate=pl.CostEstimate(flops=10 * heads * tokens * tokens * HEAD, transcendentals=heads * tokens * tokens, bytes_accessed=7 * tokens * heads * HEAD * 2),
    )(q, k, v, d_out, lse, cos, sin)


BLOCK = 256


def _params():
    return pltpu.CompilerParams(dimension_semantics=("arbitrary",), vmem_limit_bytes=44 * 2**20)


def _pair(k, n, m):
    return pl.BlockSpec((BLOCK, n), lambda i, *_: (jnp.clip(i - k * m, 0, m - 1), 0))


def _kept(shape):
    return pl.BlockSpec(shape, lambda i, *_: (0, 0), pipeline_mode=pl.Buffered(1))


def _cost(flops, arrays):
    return pl.CostEstimate(flops=flops, transcendentals=0, bytes_accessed=sum(a.size * a.dtype.itemsize for a in arrays))


def _rows_kernel(pos_ref, *refs, work, m, n_in, n_w, n_out):
    for k in range(n_in):

        @pl.when(pl.program_id(0) // m == k)
        def _(k=k):
            work(refs[k], refs[n_in : n_in + n_w], refs[-n_out:], pos_ref)


def rows_into(work, arrays, weights, places, total, widths, buffers=None, flops=0):
    rows, n_in = arrays[0].shape[0], len(arrays)
    m = rows // BLOCK
    pos = jnp.stack([jnp.asarray(p, jnp.int32) for p in places])
    out = lambda n: pl.BlockSpec((BLOCK, n), lambda i, pos: (pos[i // m] * m + i % m, 0))
    given = list(buffers or ())
    return pl.pallas_call(
        functools.partial(_rows_kernel, work=work, m=m, n_in=n_in, n_w=len(weights), n_out=len(widths)),
        grid_spec=pltpu.PrefetchScalarGridSpec(
            num_scalar_prefetch=1,
            grid=(n_in * m,),
            in_specs=[*(_pair(k, a.shape[1], m) for k, a in enumerate(arrays)), *(_kept(w.shape) for w in weights), *(pl.BlockSpec(memory_space=pl.ANY) for _ in given)],
            out_specs=[out(n) for n in widths],
        ),
        out_shape=[jax.ShapeDtypeStruct((total, n), jnp.bfloat16) for n in widths],
        input_output_aliases={1 + n_in + len(weights) + i: i for i in range(len(given))},
        compiler_params=_params(),
        cost_estimate=_cost(flops, [*arrays, *weights]),
    )(pos, *arrays, *weights, *given)


def bf16(t):
    return t.astype(jnp.bfloat16)


def f32(t):
    return t.astype(jnp.float32)


def _project(a_ref, w_refs, outs, pos_ref):
    k = w_refs[0].shape[0]
    for out, first, second in zip(outs, w_refs[::2], w_refs[1::2]):
        out[...] = bf16(_dot(a_ref[:, :k], first[...], 1, 0) + _dot(a_ref[:, k:], second[...], 1, 0))
    outs[-2][...], outs[-1][...] = a_ref[:, :k], a_ref[:, k:]


def _hidden_back_kernel(a_ref, b_ref, w_ref, *rest, m):
    out_ref, copy_ref = rest[-2:]

    def work(x_ref):
        out_ref[...] = bf16(_dot(x_ref[...], w_ref[...], 1, 1))
        copy_ref[...] = x_ref[...]

    @pl.when(pl.program_id(0) < m)
    def _():
        work(a_ref)

    @pl.when(pl.program_id(0) >= m)
    def _():
        work(b_ref)


def hidden_back(a, b, w, n, total, buffer):
    rows, d = a.shape
    m = rows // BLOCK
    given = [] if buffer is None else [buffer]
    return pl.pallas_call(
        functools.partial(_hidden_back_kernel, m=m),
        grid=(2 * m,),
        in_specs=[_pair(0, d, m), _pair(1, d, m), _kept(w.shape), *(pl.BlockSpec(memory_space=pl.ANY) for _ in given)],
        out_specs=[pl.BlockSpec((BLOCK, w.shape[0]), lambda i: (i, 0)), pl.BlockSpec((BLOCK, d), lambda i: (n * 2 * m + i, 0))],
        out_shape=[jax.ShapeDtypeStruct((2 * rows, w.shape[0]), jnp.bfloat16), jax.ShapeDtypeStruct((total, d), jnp.bfloat16)],
        input_output_aliases={3: 1} if given else {},
        compiler_params=_params(),
        cost_estimate=_cost(4 * rows * d * w.shape[0], [a, b, w]),
    )(a, b, w, *given)


def _heads_back(a_ref, w_refs, outs, pos_ref):
    a = a_ref[...]
    n = w_refs[0].shape[0]
    for j, w in enumerate(w_refs):
        place = pos_ref[4] if j == 0 else 1 - pos_ref[4]
        outs[0][:, pl.ds(pl.multiple_of(place * n, n), n)] = bf16(_dot(a, w[...], 1, 1))
    outs[1][...] = a


def _from_kernel(pos_ref, *refs, turned, n_in, n_w):
    ins, w_refs, outs = refs[:n_in], refs[n_in : n_in + n_w], refs[n_in + n_w :]

    def put(o_ref):
        if turned:
            n = w_refs[0].shape[0]
            for j in range(2):
                o_ref[:, j * n : (j + 1) * n] = bf16(sum(_dot(a[...], w[...], 1, 1) for a, w in zip(ins, w_refs[j::2])))
        else:
            o_ref[...] = bf16(sum(_dot(a[...], w[...], 1, 0) for a, w in zip(ins, w_refs)))

    m = pl.num_programs(0) // len(outs)
    for k, o_ref in enumerate(outs):

        @pl.when(pl.program_id(0) // m == k)
        def _(o_ref=o_ref):
            put(o_ref)


def rows_from(t, weights, places, rows, width, order=None):
    m, n = rows // BLOCK, len(places)
    turned = order is None
    pos = jnp.stack([jnp.asarray(p, jnp.int32) for p in (*places, 0 if turned else order)])
    parts = len(weights) // 2 if turned else 2
    wide = t.shape[1] // parts
    column = lambda j, pos: j if turned else pos[n] if j == 0 else 1 - pos[n]
    ins = [pl.BlockSpec((BLOCK, wide), lambda i, pos, j=j: (pos[i // m] * m + i % m, column(j, pos))) for j in range(parts)]
    return pl.pallas_call(
        functools.partial(_from_kernel, turned=turned, n_in=parts, n_w=len(weights)),
        grid_spec=pltpu.PrefetchScalarGridSpec(
            num_scalar_prefetch=1,
            grid=(n * m,),
            in_specs=[*ins, *(_kept(w.shape) for w in weights)],
            out_specs=[_pair(k, width, m) for k in range(n)],
        ),
        out_shape=[jax.ShapeDtypeStruct((rows, width), jnp.bfloat16)] * n,
        compiler_params=_params(),
        cost_estimate=_cost(2 * n * rows * sum(w.size for w in weights), weights),
    )(pos, *([t] * parts), *weights)


def _place_kernel(d_ref, *refs):
    d = d_ref[0]
    for out, u, v in zip(refs[4:], refs[:2], refs[2:4]):
        n = u.shape[1]
        out[:, pl.ds(pl.multiple_of(d * n, n), n)] = u[...]
        out[:, pl.ds(pl.multiple_of((1 - d) * n, n), n)] = v[...]


def placed(own, other, d):
    rows, n = own[0].shape
    spec = lambda w: pl.BlockSpec((BLOCK, w), lambda i, _: (i, 0))
    return pl.pallas_call(
        _place_kernel,
        grid_spec=pltpu.PrefetchScalarGridSpec(num_scalar_prefetch=1, grid=(rows // BLOCK,), in_specs=[spec(n)] * 4, out_specs=[spec(2 * n)] * 2),
        out_shape=[jax.ShapeDtypeStruct((rows, 2 * n), jnp.bfloat16)] * 2,
        compiler_params=_params(),
        cost_estimate=_cost(0, [*own, *other, *own, *other]),
    )(jnp.asarray(d, jnp.int32).reshape(1), *own, *other)


def _ffn_kernel(a_ref, b_ref, *rest, piece, m, swapped, n_back, n_given):
    back, rest = rest[:n_back], rest[n_back:]
    hbm, rest = rest[: n_back + 1], rest[n_back + 1 + n_given :]
    hid_ref, dg_ref, du_ref, lo_ref, hi_ref = rest[:5]
    dy_ref = rest[5]
    da_ref, db_ref = rest[3 + n_back + 1 : 3 + n_back + 3]
    *held, sems = rest[3 + n_back + 3 :]
    w1_ref, w2_ref = held[:2]
    k, units = w1_ref.shape[0], w1_ref.shape[1] // 2
    cuts = [(at, piece) for at in range(0, units, piece)]
    opening = [(0, piece // 3), (piece // 3, piece - piece // 3), *cuts[1:]]

    def copies(p, at, piece):
        for j in range(4):
            here = (slice(None), slice(at + j // 2 * units, at + j // 2 * units + piece))
            yield pltpu.make_async_copy(hbm[j % 2].at[here], held[j % 2].at[here], sems.at[5 * p + j])
        if n_back == 2:
            here = slice(at, at + piece)
            yield pltpu.make_async_copy(hbm[2].at[here], held[2].at[here], sems.at[5 * p + 4])

    def work(x_ref, back_ref, dx_ref, first):
        x1, x2 = x_ref[:, :k], x_ref[:, k:]
        lo_ref[...], hi_ref[...] = x1, x2
        if n_back == 2:
            dy_ref[...] = back_ref[...]
        for p, (at, piece) in enumerate(opening if first else cuts):
            if first:
                for copy in copies(p, at, piece):
                    copy.wait()
            here, there = slice(at, at + piece), slice(units + at, units + at + piece)
            g = _dot(x1, w1_ref[:, here], 1, 0) + _dot(x2, w2_ref[:, here], 1, 0)
            u = _dot(x1, w1_ref[:, there], 1, 0) + _dot(x2, w2_ref[:, there], 1, 0)
            dh = f32(bf16(_dot(back_ref[...], held[2][here, :], 1, 1)) if n_back == 2 else back_ref[:, here])
            s = jax.nn.sigmoid(g)
            gs = g * s
            hid_ref[:, here] = bf16(gs * u)
            dg_ref[:, here] = bf16(dh * u * (s + gs * (1 - s)))
            du_ref[:, here] = bf16(dh * gs)
        for j, w in enumerate((w2_ref, w1_ref) if swapped else (w1_ref, w2_ref)):
            dx_ref[:, j * k : (j + 1) * k] = bf16(_dot(dg_ref[...], w[:, :units], 1, 1) + _dot(du_ref[...], w[:, units:], 1, 1))

    @pl.when(pl.program_id(0) == 0)
    def _():
        for p, (at, piece) in enumerate(opening):
            for copy in copies(p, at, piece):
                copy.start()
        work(a_ref, back[0], da_ref, True)

    @pl.when((pl.program_id(0) > 0) & (pl.program_id(0) < m))
    def _():
        work(a_ref, back[0], da_ref, False)

    @pl.when(pl.program_id(0) >= m)
    def _():
        work(b_ref, back[-1], db_ref, False)


def ffn(a, b, back, weights, n, total, buffers, swapped, piece=768):
    rows, d = a.shape
    units = weights[0].shape[1] // 2
    m = rows // BLOCK
    at = lambda width: pl.BlockSpec((BLOCK, width), lambda i: (n * 2 * m + i, 0))
    anywhere = pl.BlockSpec(memory_space=pl.ANY)
    two = len(back) == 2
    backs = [_pair(0, d, m), _pair(1, d, m)] if two else [pl.BlockSpec((BLOCK, units), lambda i: (i, 0))]
    given = list(buffers or ())
    widths = (units, units, units, d // 2, d // 2) + ((d,) if two else ())
    first = 2 + len(back) + len(weights)
    *buffers, da, db = pl.pallas_call(
        functools.partial(_ffn_kernel, piece=piece, m=m, swapped=swapped, n_back=len(back), n_given=len(given)),
        grid=(2 * m,),
        in_specs=[_pair(0, d, m), _pair(1, d, m), *backs, *[anywhere] * (len(weights) + len(given))],
        out_specs=[*(at(w) for w in widths), _pair(0, d, m), _pair(1, d, m)],
        out_shape=[*(jax.ShapeDtypeStruct((total, w), jnp.bfloat16) for w in widths), *[jax.ShapeDtypeStruct((rows, d), jnp.bfloat16)] * 2],
        input_output_aliases={first + i: i for i in range(len(given))},
        scratch_shapes=[*(pltpu.VMEM(w.shape, w.dtype) for w in weights), pltpu.SemaphoreType.DMA((5 * (units // piece + 1),))],
        compiler_params=_params(),
        cost_estimate=_cost((20 if two else 16) * rows * d * units, [a, b, *weights]),
    )(a, b, *back, *weights, *given)
    return buffers, da, db


def normed(h):
    wide = f32(h)
    scale = lax.rsqrt(jnp.mean(wide**2, -1, keepdims=True) + 1e-6)
    return bf16(wide * scale)


def normed_bwd(h, by):
    wide, by = f32(h), f32(by)
    scale = lax.rsqrt(jnp.mean(wide**2, -1, keepdims=True) + 1e-6)
    return scale * (by - wide * (scale * scale * jnp.mean(by * wide, -1, keepdims=True)))


CORE, OVER_X, OVER_Y = ("tp", ((0, 1), (1, 0), (2, 3), (3, 2))), ("tp", ((0, 2), (1, 3), (2, 0), (3, 1))), ("dp", ((0, 1), (1, 0)))


ACROSS = (("dp", "tp"), tuple((i, (i + 4) % 8 // 4 * 4 + (i + 2) % 4) for i in range(8)))


def send(way, t):
    return lax.ppermute(t, way[0], way[1])


def layer(x, dy, wq, wk, wv, wo, wg, wu, wd):
    d, t = lax.axis_index("dp"), lax.axis_index("tp")
    own, width = x.shape
    seq, units = 4 * own, wd.shape[0]
    half = width // 2
    t_core, t_x = t + 1 - 2 * lax.rem(t, 2), lax.rem(t + 2, 4)
    t_xcore = t_x + 1 - 2 * lax.rem(t, 2)
    ordered = lambda t, place: jnp.where(place == 0, t, jnp.concatenate([t[:, half:], t[:, :half]], 1))
    mine = lambda w: lax.dynamic_slice_in_dim(w, d * units, units, axis=1)
    theirs = lambda w: lax.dynamic_slice_in_dim(w, (1 - d) * units, units, axis=1)

    w_qkv = []
    for w in (wq, wk, wv):
        w_qkv += [w, send(OVER_Y, w)]
    a = ordered(normed(x), d)
    ax = send(OVER_X, a)
    ac = send(CORE, a)
    gu_send = jnp.concatenate([theirs(wg), theirs(wu)], 1)
    gu_mine = jnp.concatenate([mine(wg), mine(wu)], 1)
    wo_theirs = send(OVER_Y, wo)
    gu_theirs = send(OVER_Y, gu_send)
    axc = send(CORE, ax)

    dyc = send(CORE, dy)
    dyx = send(OVER_X, dy)
    dyxc = send(CORE, dyx)
    dyy = send(OVER_Y, dy)
    dyyc = send(CORE, dyy)
    dyd = send(OVER_X, dyy)
    dydc = send(CORE, dyd)

    angle = jnp.arange(seq, dtype=jnp.float32)[:, None] * THETA ** (-jnp.arange(HALF, dtype=jnp.float32) / HALF)
    cos, sin = jnp.cos(angle), jnp.sin(angle)

    cols = wq.shape[1]
    proj = functools.partial(rows_into, _project, weights=w_qkv, total=seq, widths=(cols, cols, cols, half, half), flops=12 * own * width * cols)
    kept = proj([a, ac], places=(t, t_core))
    *qkv, a_lo, a_hi = proj([ax, axc], places=(t_x, t_xcore), buffers=kept)
    heads, lse = attend(*qkv, cos, sin)
    o_from = functools.partial(rows_from, heads, [wo, wo_theirs], rows=own, width=width, order=d)
    ox, oxc = o_from(places=(t_x, t_xcore))
    sox = bf16(f32(ox) + f32(send(CORE, oxc)))
    o_far = send(OVER_X, sox)
    o, oc = o_from(places=(t, t_core))
    o_near = send(CORE, oc)
    h = bf16(f32(x) + f32(bf16(f32(o) + f32(o_near) + f32(o_far))))
    b = normed(h)
    b_mine, b_other = ordered(b, d), ordered(b, 1 - d)

    by = send(OVER_Y, b_other)
    bx = send(OVER_X, b_mine)
    bc = send(CORE, b_mine)
    bxc = send(CORE, bx)
    byc = send(CORE, by)
    bd = send(OVER_X, by)
    bdc = send(CORE, bd)
    dy_all, kept, sums = None, None, []
    given = ((dy, dyc, b_mine, bc), (dyx, dyxc, bx, bxc), (dyy, dyyc, by, byc), (dyd, dydc, bd, bdc))
    for n, (dy_u, dy_v, u, v) in enumerate(given):
        if n < 2:
            d_hid, dy_all = hidden_back(dy_u, dy_v, wd, n, 2 * seq, dy_all)
            back, weights = [d_hid], [gu_mine, gu_theirs]
        else:
            back, weights = [dy_u, dy_v], [gu_mine, gu_theirs, wd]
            kept = [*kept, dy_all] if n == 2 else kept
        kept, du, dv = ffn(u, v, back, weights, n, 2 * seq, kept, n >= 2)
        near = send(CORE, dv)
        total = f32(du) + f32(near)
        sums.append(bf16(total) if n else total)
    hid, dg, du, b_lo, b_hi, dy_all = kept
    from_x = send(OVER_X, sums[1])
    from_y = send(OVER_Y, sums[2])
    from_d = send(ACROSS, sums[3])
    db = bf16(ordered(sums[0] + f32(from_x) + f32(from_y) + f32(from_d), d))
    dh = bf16(f32(dy) + f32(bf16(normed_bwd(h, db))))

    got_gu, kept_gu = [], []
    for g in (dg, du):
        part = bf16(_dot(b_hi, g, 0, 0))
        got_gu.append(send(OVER_Y, part))
        kept_gu.append(bf16(_dot(b_lo, g, 0, 0)))
    d_wd = bf16(_dot(hid, dy_all, 0, 0))

    dhx = send(OVER_X, dh)
    dhc = send(CORE, dh)
    dhxc = send(CORE, dhx)
    heads_back = functools.partial(rows_into, _heads_back, weights=(wo, wo_theirs), total=seq, widths=(heads.shape[1], width), flops=8 * own * width * heads.shape[1])
    d_heads, dh_all = heads_back([dh, dhc, dhx, dhxc], places=(t, t_core, t_x, t_xcore, d))
    d_qkv = attend_bwd(*qkv, d_heads, lse, cos, sin)
    part = bf16(_dot(a_hi, d_qkv, 0, 0))
    got = send(OVER_Y, part)
    dax, daxc, da, dac = rows_from(d_qkv, w_qkv, (t_x, t_xcore, t, t_core), own, width)
    sdax = bf16(f32(dax) + f32(send(CORE, daxc)))
    da_far = send(OVER_X, sdax)
    da_near = send(CORE, dac)
    d_wo_all = bf16(_dot(heads, dh_all, 0, 0))
    rows = wo.shape[0]
    wo_part = lambda i: lax.dynamic_slice_in_dim(d_wo_all, i * rows, rows, axis=0)
    wo_send = wo_part(1 - d)
    wo_got = send(OVER_Y, wo_send)
    part_kept = lax.optimization_barrier(_dot(a_lo, d_qkv, 0, 0))
    d_wg, d_wu = placed(kept_gu, got_gu, d)
    da_sum = bf16(ordered(f32(da) + f32(da_near) + f32(da_far), d))
    dx = bf16(f32(dh) + f32(bf16(normed_bwd(x, da_sum))))
    d_w_qkv = [bf16(part_kept[:, i : i + cols] + f32(got[:, i : i + cols])) for i in range(0, 3 * cols, cols)]
    d_wo = bf16(f32(wo_part(d)) + f32(wo_got))
    return dx, *d_w_qkv, d_wo, d_wg, d_wu, d_wd


def solution(mesh):
    def step(x, dy, *weights):
        dx, *rest = layer(x[0], dy[0], *weights)
        return (dx[None], *rest)

    states, by_columns, by_rows = P("dp", "tp", None), P("dp", "tp"), P(("tp", "dp"), None)
    weights = (by_columns, by_columns, by_columns, by_rows, by_columns, by_columns, by_rows)
    return jax.shard_map(step, mesh=mesh, in_specs=(states, states, *weights), out_specs=(states, *weights), check_vma=False)
```
